128 devices in a mesh: rows: 128 (over y, x, z, core).
Axes of the slice: x: 4, y: 4, z: 4, core: 2. Of those that a mesh axis runs over, the one named last changes fastest.
Arguments:
- blocks: float32 [2048, 4, 256, 256], P('rows'), may hold values from -0.125 to 0.125
- block_cols: int32 [2048, 4], P('rows'), may hold values from 0 to 2047, as said below
- live_counts: int32 [2048], P('rows'), may hold values from 1 to 4, as said below
- onsite_energy: float32 [524288], P('rows'), may hold values from -2 to 2
- precond: float32 [2048, 256, 256], P('rows')
- vectors: float32 [32, 524288], P(None, 'rows'), may hold values from -6 to 6
- prev_vectors: float32 [32, 524288], P(None, 'rows'), may hold values from -6 to 6
- prev_image: float32 [32, 524288], P(None, 'rows'), may hold values from -6 to 6
Outputs:
- correction: float32 [32, 524288], P(None, 'rows')
- reduced: float32 [96, 96], replicated
The draws below stay inside these ranges and needn't reach their ends.
Inputs may be any that keep to these rules, and one draw needn't show every extreme that they name: block_cols[b, s] = (b + o) mod 2048, with the offsets o of one block-row distinct and within 0 to 4; every slot holds a valid block-column. Slots s < live_counts[b] are live, the rest are ignored; some block-row has 4 live slots in every draw.
All inputs are finite; a program needn't handle non-finite values.
Results may differ from the reference program's by a relative error of at most 0.00026.
Values sent between devices are 32-bit elements; how exact they have to be, the bound alone decides.
A program may use at most 128 MiB of HBM per device.

```python
import jax
import jax.numpy as jnp
from jax import lax

BS = 256
K = 32
BR_DEV = 16
HB = 4
MAXB = 4
ITERS = 3
NBR = 2048
NROWS = 524288
BASIS = 96


def draw_block_cols(key, part):
    scores = jax.random.randint(key, (NBR, HB + 1), 0, 1 << 20) * (HB + 1) + jnp.arange(HB + 1, dtype=jnp.int32)[None, :]
    offsets = jnp.argsort(scores, axis=1)[:, :MAXB].astype(jnp.int32)
    return ((jnp.arange(NBR, dtype=jnp.int32)[:, None] + offsets) % NBR).astype(jnp.int32)


def draw_live_counts(key, part):
    first_key = jax.random.fold_in(key, 11)
    second_key = jax.random.fold_in(key, 23)
    third_key = jax.random.fold_in(key, 37)
    shifts = jax.random.randint(first_key, (NBR // BR_DEV,), 0, 3)
    ceiling = jnp.maximum(jnp.right_shift(jnp.full((NBR // BR_DEV,), MAXB, jnp.int32), shifts), 1)
    ceiling_rows = jnp.repeat(ceiling, BR_DEV)
    uniform_ints = jax.random.randint(second_key, (NBR,), 0, 1024)
    counts = 1 + uniform_ints * ceiling_rows // 1024
    position = jax.random.randint(third_key, (), 0, NBR)
    return counts.at[position].set(MAXB).astype(jnp.int32)


def draw_precond(key, part):
    noise = jax.random.normal(key, (NBR, BS, BS), jnp.float32)
    return jnp.eye(BS, dtype=jnp.float32)[None, :, :] + 0.5 * noise / jnp.sqrt(jnp.float32(BS))


def level_of(own_key, extent, shards, least, largest):
    def one(dim, shards_of):
        steps = jax.random.uniform(jax.random.fold_in(jax.random.fold_in(own_key, 6), dim), (shards_of,), jnp.float32, least / len(shards), largest / len(shards))
        return jnp.repeat(jnp.exp(steps), extent[dim] // shards_of).reshape((-1,) + (1,) * (len(extent) - dim - 1))

    loudness = one(*shards[0])
    for cut in shards[1:]:
        loudness = loudness * one(*cut)
    return loudness


def normal_values(key, extent, scale, reach, split=(), kind=jnp.bfloat16):
    drawn = scale * jax.random.normal(key, extent, jnp.float32)
    if split:
        drawn = drawn * level_of(key, extent, split, -0.22, 0.18)
    return jnp.clip(drawn, -reach, reach).astype(kind)


def setup_inputs(seed: int = 0) -> dict:
    seeds = jax.random.split(jax.random.key(seed), 9)
    return {
        "blocks": normal_values(seeds[0], (NBR, MAXB, BS, BS), (2 * MAXB * BS) ** -0.5, 0.125, ((0, 128),), jnp.float32),
        "block_cols": draw_block_cols(jax.random.fold_in(seeds[8], 71), 0),
        "live_counts": draw_live_counts(jax.random.fold_in(seeds[8], 71), 0),
        "onsite_energy": jnp.clip(jax.random.uniform(seeds[3], (NROWS,), jnp.float32, -2.0, 2.0) * level_of(seeds[3], (NROWS,), ((0, 128),), -0.4, 0.0), -2.0, 2.0),
        "precond": draw_precond(jax.random.fold_in(seeds[8], 71), 0),
        "vectors": normal_values(seeds[5], (K, NROWS), 1.0, 6.0, ((1, 128),), jnp.float32),
        "prev_vectors": normal_values(seeds[6], (K, NROWS), 1.0, 6.0, ((1, 128),), jnp.float32),
        "prev_image": normal_values(seeds[7], (K, NROWS), 1.0, 6.0, ((1, 128),), jnp.float32),
    }


def operate(field, blocks, block_cols, live_mask, onsite_energy):
    vec_count = field.shape[0]
    source = field.reshape(vec_count, NBR, BS)
    picked = source[:, block_cols] * live_mask[None, :, :, None]
    forward_part = jnp.einsum('bsij,kbsj->kbi', blocks, picked, precision=lax.Precision.HIGHEST)
    moved = jnp.einsum('kbi,bsij->kbsj', source, blocks, precision=lax.Precision.HIGHEST) * live_mask[None, :, :, None]
    spread = jnp.zeros_like(source).at[:, block_cols].add(moved)
    return onsite_energy[None, :] * field + (forward_part + spread).reshape(vec_count, -1)

def reference(blocks, block_cols, live_counts, onsite_energy, precond, vectors, prev_vectors, prev_image):
    live_mask = (jnp.arange(MAXB, dtype=jnp.int32)[None, :] < live_counts[:, None]).astype(jnp.float32)
    image = operate(vectors, blocks, block_cols, live_mask, onsite_energy)
    quotient = jnp.sum(vectors * image, axis=1) / jnp.sum(vectors * vectors, axis=1)
    remainder = -(image - quotient[:, None] * vectors)
    correction = jnp.zeros_like(vectors)
    hcorr = jnp.zeros_like(vectors)
    for iteration in range(ITERS):
        search = jnp.einsum('bij,kbj->kbi', precond, remainder.reshape(K, NBR, BS), precision=lax.Precision.HIGHEST).reshape(K, -1)
        applied = operate(search, blocks, block_cols, live_mask, onsite_energy) - quotient[:, None] * search
        step_size = jnp.sum(applied * remainder, axis=1) / (jnp.sum(applied * applied, axis=1) + 1.0)
        correction = correction + step_size[:, None] * search
        hcorr = hcorr + step_size[:, None] * (applied + quotient[:, None] * search)
        remainder = remainder - step_size[:, None] * applied
    basis = jnp.concatenate([vectors, prev_vectors, correction], axis=0)
    himage = jnp.concatenate([image, prev_image, hcorr], axis=0)
    gram_matrix = jnp.dot(basis, basis.T, precision=lax.Precision.HIGHEST) + jnp.eye(BASIS, dtype=jnp.float32)
    projected = jnp.dot(basis, himage.T, precision=lax.Precision.HIGHEST)
    factor = jnp.linalg.cholesky(gram_matrix)
    half_way = jax.scipy.linalg.solve_triangular(factor, projected, lower=True)
    reduced = jax.scipy.linalg.solve_triangular(factor, half_way.T, lower=True).T
    return (correction, reduced)
```

```python
import jax
import jax.numpy as jnp
from jax import lax
from jax.experimental import pallas as pl
from jax.experimental.pallas import tpu as pltpu
from jax.sharding import PartitionSpec as P

MESH = pl.DeviceIdType.MESH
F32 = jnp.float32
BF16 = jnp.bfloat16
HB = 4
ITERS = 3
LOW = 8
SLOTS = 4
STAGES = 4


def split(x):
    high = x.astype(BF16)
    return high, (x - high.astype(F32)).astype(BF16)


def mm(a, b):
    return jnp.dot(a, b, preferred_element_type=F32)


def mmt(a, b):
    return lax.dot_general(a, b, (((1,), (1,)), ((), ())), preferred_element_type=F32)


def kernel(
    n_dev, rows, kvec, bs,
    cols, live, blocks, onsite, precond, vec, pvec, pimg,
    corr, mats,
    stage, bh, bl, ph, plo, offs,
    fv, fpv, fpi, fim, fr, fu, fhu, fa, fz, fc, fh, zs, acc, qb, sb,
    zhalo, inc, spill, red1, red2, gram, parts, big1, big2, fin,
    stage_sem, load_sem, out_sem, zs_sem, zr_sem, ss_sem, sr_sem,
    r1s, r1r, r2s, r2r, b1s, b1r, b2s, b2r, b3s, b3r,
):
    me = lax.axis_index("rows")
    low = lax.rem(me, LOW)
    high = lax.div(me, LOW)
    n_high = n_dev // LOW
    total = n_dev * rows
    first = me * rows
    right = lax.rem(me + 1, n_dev)
    left = lax.rem(me + n_dev - 1, n_dev)
    edge = rows - HB
    order = list(range(edge, rows)) + list(range(edge))

    def load_field(src, dst, sem):
        for b in range(rows):
            pltpu.make_async_copy(src.at[:, pl.ds(b * bs, bs)], dst.at[b], sem).start()

    def load_wait(dst, sem):
        pltpu.make_async_copy(dst, dst, sem).wait()

    n_chunks = rows + rows // SLOTS

    def chunk(i):
        slot = i % STAGES
        if i < rows:
            src = blocks.at[order[i]]
        else:
            src = precond.at[pl.ds((i - rows) * SLOTS, SLOTS)]
        return pltpu.make_async_copy(src, stage.at[slot], stage_sem.at[slot])

    load_field(vec, fv, load_sem.at[0])
    for i in range(STAGES):
        chunk(i).start()

    barrier = pltpu.get_barrier_semaphore()
    peers = [left, right]
    peers += [high * LOW + lax.rem(low + j, LOW) for j in range(1, LOW)]
    peers += [lax.rem(high + j, n_high) * LOW + low for j in range(1, n_high)]
    for peer in peers:
        pl.semaphore_signal(barrier, inc=1, device_id=(peer,), device_id_type=MESH)
    pl.semaphore_wait(barrier, len(peers))

    def rcopy(src, dst, s_sem, r_sem, to):
        return pltpu.make_async_remote_copy(
            src_ref=src, dst_ref=dst, send_sem=s_sem, recv_sem=r_sem,
            device_id=(to,), device_id_type=MESH,
        )

    def z_copy(n, field):
        return rcopy(field.at[pl.ds(0, HB)], zhalo.at[n], zs_sem.at[n], zr_sem.at[n], left)

    def spill_copy(n):
        return rcopy(spill.at[n], inc.at[n], ss_sem.at[n], sr_sem.at[n], right)

    def low_copy(i, j):
        to = high * LOW + lax.rem(low + j, LOW)
        return rcopy(red1.at[i, low], red1.at[i, low], r1s.at[i, j], r1r.at[i, low], to)

    def low_in(i, j):
        frm = lax.rem(low + j, LOW)
        return rcopy(red1.at[i, frm], red1.at[i, frm], r1s.at[i, j], r1r.at[i, frm], left)

    def high_copy(i, j):
        to = lax.rem(high + j, n_high) * LOW + low
        return rcopy(red2.at[i, high], red2.at[i, high], r2s.at[i, j], r2r.at[i, high], to)

    def high_in(i, j):
        frm = lax.rem(high + j, n_high)
        return rcopy(red2.at[i, frm], red2.at[i, frm], r2s.at[i, j], r2r.at[i, frm], left)

    lane = lax.broadcasted_iota(jnp.int32, (8, 128), 1)
    groups = kvec // 8

    def pack(a, b):
        tile = jnp.zeros((8, 128), F32)
        for g in range(groups):
            tile = tile + jnp.where(lane == g, a[8 * g:8 * g + 8], 0.0)
            tile = tile + jnp.where(lane == groups + g, b[8 * g:8 * g + 8], 0.0)
        return tile

    def unpack(tile):
        out = []
        for base in (0, groups):
            out.append(jnp.concatenate(
                [jnp.sum(jnp.where(lane == base + g, tile, 0.0), axis=1, keepdims=True) for g in range(groups)],
                axis=0,
            ))
        return out

    def red_start(i, a, b):
        red1[i, low] = pack(a, b)
        for j in range(1, LOW):
            low_copy(i, j).start()

    def red_mid(i):
        for j in range(1, LOW):
            low_in(i, j).wait_recv()
        tile = red1[i, 0]
        for l in range(1, LOW):
            tile = tile + red1[i, l]
        red2[i, high] = tile
        for j in range(1, n_high):
            high_copy(i, j).start()

    def red_end(i):
        for j in range(1, n_high):
            high_in(i, j).wait_recv()
        tile = red2[i, 0]
        for l in range(1, n_high):
            tile = tile + red2[i, l]
        for j in range(1, LOW):
            low_copy(i, j).wait_send()
        for j in range(1, n_high):
            high_copy(i, j).wait_send()
        return unpack(tile)

    def put_split(b, z):
        zh, zl = split(z)
        zs[b, 0:kvec, :] = zh
        zs[b, kvec:2 * kvec, :] = zl

    def onto(b):
        zb = zs[b]
        zh = zb[0:kvec]
        sums = [None] * (HB + 1)
        for s in range(SLOTS):
            part = mm(zb, bh[b * SLOTS + s])
            moved = part[0:kvec] + part[kvec:] + mm(zh, bl[b * SLOTS + s])
            off = offs[b * SLOTS + s]
            for o in range(HB + 1):
                term = jnp.where(off == o, 1.0, 0.0) * moved
                sums[o] = term if sums[o] is None else sums[o] + term
        for o in range(HB + 1):
            acc[b + o] = acc[b + o] + sums[o]

    def across(b):
        out = None
        for s in range(SLOTS):
            zc = zs[b + offs[b * SLOTS + s]]
            part = mmt(zc, bh[b * SLOTS + s])
            term = part[0:kvec] + part[kvec:] + mmt(zc[0:kvec], bl[b * SLOTS + s])
            out = term if out is None else out + term
        acc[b] = acc[b] + out

    def halo_in(n):
        z_copy(n, fv).wait_recv()
        for t in range(HB):
            put_split(rows + t, zhalo[n, t])

    def send_spill(n):
        for t in range(HB):
            spill[n, t] = acc[rows + t]
        spill_copy(n).start()

    def take_in(n):
        spill_copy(n).wait_recv()
        for t in range(HB):
            acc[t] = acc[t] + inc[n, t]

    def diag(b, z):
        acc[b] = onsite[b] * z

    def clear_tail():
        for t in range(HB):
            acc[rows + t] = jnp.zeros((kvec, bs), F32)

    load_wait(fv, load_sem.at[0])
    z_copy(0, fv).start()
    load_field(pvec, fpv, load_sem.at[1])
    load_field(pimg, fpi, load_sem.at[2])

    def prepare(b, c):
        z = fv[b]
        put_split(b, z)
        diag(b, z)
        return c

    lax.fori_loop(0, rows, prepare, 0)
    clear_tail()

    def take_chunk(i):
        chunk(i).wait()
        slot = i % STAGES
        if i < rows:
            b = order[i]
            for s in range(SLOTS):
                off = lax.rem(cols[b, s] - first - b + 2 * total, total)
                offs[b * SLOTS + s] = jnp.minimum(off, HB)
                alive = jnp.where(s < live[b], 1.0, 0.0)

                def piece(p, c):
                    at = pl.ds(pl.multiple_of(p * 64, 64), 64)
                    xh, xl = split(stage[slot, s, at, :] * alive)
                    bh[b * SLOTS + s, at, :] = xh
                    bl[b * SLOTS + s, at, :] = xl
                    return c

                lax.fori_loop(0, bs // 64, piece, 0)
        else:
            for s in range(SLOTS):
                def piece(p, c):
                    at = pl.ds(pl.multiple_of(p * 64, 64), 64)
                    xh, xl = split(stage[slot, s, at, :])
                    ph[(i - rows) * SLOTS + s, at, :] = xh
                    plo[(i - rows) * SLOTS + s, at, :] = xl
                    return c

                lax.fori_loop(0, bs // 64, piece, 0)
        if i + STAGES < n_chunks:
            chunk(i + STAGES).start()

    for i in range(HB):
        take_chunk(i)
        onto(order[i])
    send_spill(0)
    for i in range(HB, rows):
        take_chunk(i)
        onto(order[i])
        across(order[i])
    halo_in(0)
    for b in range(edge, rows):
        across(b)
    take_in(0)

    zero = jnp.zeros((kvec, bs), F32)

    def first_sums(b, c):
        x, im = fv[b], acc[b]
        fim[b] = im
        return c[0] + x * im, c[1] + x * x

    num, den = lax.fori_loop(0, rows, first_sums, (zero, zero))
    total_of = lambda x: jnp.sum(x, axis=1, keepdims=True)
    red_start(0, total_of(num), total_of(den))
    for i in range(rows, n_chunks):
        take_chunk(i)
    red_mid(0)
    num, den = red_end(0)
    q = num / den
    qb[...] = jnp.broadcast_to(q, (kvec, bs))

    def first_rest(b, c):
        fr[b] = qb[...] * fv[b] - fim[b]
        return c

    lax.fori_loop(0, rows, first_rest, 0)

    def precondition(field, b):
        dh, dl = split(field[b])
        both = jnp.concatenate([dh, dl], axis=0)
        part = mmt(both, ph[b])
        z = part[0:kvec] + part[kvec:] + mmt(dh, plo[b])
        fz[b] = z
        put_split(b, z)
        diag(b, z)

    for k in range(ITERS):
        n = k + 1
        field = fr if k == 0 else fa
        for b in range(HB):
            precondition(field, b)
        z_copy(n, fz).start()
        clear_tail()
        for b in range(edge, rows):
            precondition(field, b)
        for b in range(edge, rows):
            onto(b)
        send_spill(n)

        def interior(g, c, field=field):
            for t in range(4):
                precondition(field, 4 + 4 * g + t)
            return c

        lax.fori_loop(0, (edge - HB) // 4, interior, 0)
        if k > 0:
            red_mid(k)

        def body(g, c):
            for t in range(4):
                onto(4 * g + t)
            for t in range(4):
                across(4 * g + t)
            return c

        lax.fori_loop(0, edge // 4, body, 0)
        halo_in(n)
        for b in range(edge, rows):
            across(b)
        take_in(n)
        z_copy(n, fz).wait_send()
        if k > 0:
            cross, own = red_end(k)
            step = cross / (own + 1.0)
            sb[...] = jnp.broadcast_to(step, (kvec, bs))

        def update(b, c, k=k):
            z, hz = fz[b], acc[b]
            m = hz - qb[...] * z
            if k == 0:
                r = fr[b]
                a = m
                fu[b] = z
                fhu[b] = hz
            else:
                s = sb[...]
                u, hu, a = fu[b], fhu[b], fa[b]
                r = fr[b] - s * a
                fr[b] = r
                if k == 1:
                    fc[b] = s * u
                    fh[b] = s * hu
                else:
                    fc[b] = fc[b] + s * u
                    fh[b] = fh[b] + s * hu
                a = a - s * m
                fu[b] = u - s * z
                fhu[b] = hu - s * hz
            fa[b] = a
            return c[0] + a * r, c[1] + a * a

        cross, own = lax.fori_loop(0, rows, update, (zero, zero))
        if k + 1 < ITERS:
            red_start(k + 1, total_of(cross), total_of(own))

    load_wait(fpv, load_sem.at[1])
    load_wait(fpi, load_sem.at[2])
    gram[...] = jnp.zeros_like(gram)

    def products(b, c):
        xh, xl = split(jnp.concatenate([fv[b], fpv[b], fc[b], fu[b]], axis=0))
        yh, yl = split(jnp.concatenate([fim[b], fpi[b], fh[b], fhu[b]], axis=0))
        part = mmt(jnp.concatenate([xh, xl], axis=0), jnp.concatenate([xh, yh], axis=0))
        m = xh.shape[0]
        gram[...] = gram[...] + (part[0:m] + part[m:] + mmt(xh, jnp.concatenate([xl, yl], axis=0)))
        return c

    lax.fori_loop(0, rows, products, 0)
    wide = lax.broadcasted_iota(jnp.int32, (kvec, 128), 1)
    for p in range(4):
        at = pl.ds(p * kvec, kvec)
        g = gram[at, 0:128]
        if p == 0:
            g = jnp.where(wide == 96, total_of(cross), jnp.where(wide == 97, total_of(own), g))
        parts[p] = g
        parts[4 + p] = gram[at, 128:256]

    def big1_copy(j):
        to = lax.rem(low + j, LOW)
        return rcopy(parts.at[to], big1.at[low], b1s.at[j], b1r.at[low], high * LOW + to)

    def big1_in(j):
        frm = lax.rem(low + j, LOW)
        return rcopy(parts.at[frm], big1.at[frm], b1s.at[j], b1r.at[frm], left)

    def big2_copy(j):
        to = lax.rem(high + j, n_high) * LOW + low
        return rcopy(big2.at[high], big2.at[high], b2s.at[j], b2r.at[high], to)

    def big2_in(j):
        frm = lax.rem(high + j, n_high)
        return rcopy(big2.at[frm], big2.at[frm], b2s.at[j], b2r.at[frm], left)

    def fin_copy(j):
        to = high * LOW + lax.rem(low + j, LOW)
        return rcopy(fin.at[low], fin.at[low], b3s.at[j], b3r.at[low], to)

    def fin_in(j):
        frm = lax.rem(low + j, LOW)
        return rcopy(fin.at[frm], fin.at[frm], b3s.at[j], b3r.at[frm], left)

    for j in range(1, LOW):
        big1_copy(j).start()
    big1[low] = parts[low]
    for j in range(1, LOW):
        big1_in(j).wait_recv()
    tile = big1[0]
    for l in range(1, LOW):
        tile = tile + big1[l]
    big2[high] = tile
    for j in range(1, n_high):
        big2_copy(j).start()
    for j in range(1, n_high):
        big2_in(j).wait_recv()
    tile = big2[0]
    for l in range(1, n_high):
        tile = tile + big2[l]
    fin[low] = tile
    for j in range(1, LOW):
        fin_copy(j).start()
    for j in range(1, LOW):
        fin_in(j).wait_recv()

    head = fin[0]
    step = head[:, 96:97] / (head[:, 97:98] + 1.0)
    sb[...] = jnp.broadcast_to(step, (kvec, bs))

    def finish(b, c):
        fc[b] = fc[b] + sb[...] * fu[b]
        return c

    lax.fori_loop(0, rows, finish, 0)
    for b in range(rows):
        pltpu.make_async_copy(fc.at[b], corr.at[:, pl.ds(b * bs, bs)], out_sem).start()
    for p in range(8):
        mats[p] = fin[p]
    pltpu.make_async_copy(fc, fc, out_sem).wait()

    for j in range(1, LOW):
        big1_copy(j).wait_send()
        fin_copy(j).wait_send()
    for j in range(1, n_high):
        big2_copy(j).wait_send()
    z_copy(0, fv).wait_send()
    for n in range(ITERS + 1):
        spill_copy(n).wait_send()


def local(n_dev, blocks, block_cols, live_counts, onsite_energy, precond, vectors, prev_vectors, prev_image):
    rows, slots, bs = blocks.shape[0], blocks.shape[1], blocks.shape[2]
    kvec = vectors.shape[0]
    n_high = n_dev // LOW
    field = pltpu.VMEM((rows, kvec, bs), F32)
    dma = pltpu.SemaphoreType.DMA
    hbm = pl.BlockSpec(memory_space=pl.ANY)
    smem = pl.BlockSpec(memory_space=pltpu.SMEM)
    vmem = pl.BlockSpec(memory_space=pltpu.VMEM)

    def run(*args):
        return kernel(n_dev, rows, kvec, bs, *args)

    correction, mats = pl.pallas_call(
        run,
        out_shape=(
            jax.ShapeDtypeStruct(vectors.shape, F32),
            jax.ShapeDtypeStruct((8, kvec, 128), F32),
        ),
        in_specs=[smem, smem, hbm, vmem, hbm, hbm, hbm, hbm],
        out_specs=(hbm, vmem),
        scratch_shapes=[
            pltpu.VMEM((STAGES, slots, bs, bs), F32),
            pltpu.VMEM((rows * slots, bs, bs), BF16),
            pltpu.VMEM((rows * slots, bs, bs), BF16),
            pltpu.VMEM((rows, bs, bs), BF16),
            pltpu.VMEM((rows, bs, bs), BF16),
            pltpu.SMEM((rows * slots,), jnp.int32),
            field, field, field, field, field, field, field, field, field, field, field,
            pltpu.VMEM((rows + HB, 2 * kvec, bs), BF16),
            pltpu.VMEM((rows + HB, kvec, bs), F32),
            pltpu.VMEM((kvec, bs), F32),
            pltpu.VMEM((kvec, bs), F32),
            pltpu.VMEM((ITERS + 1, HB, kvec, bs), F32),
            pltpu.VMEM((ITERS + 1, HB, kvec, bs), F32),
            pltpu.VMEM((ITERS + 1, HB, kvec, bs), F32),
            pltpu.VMEM((ITERS, LOW, 8, 128), F32),
            pltpu.VMEM((ITERS, n_high, 8, 128), F32),
            pltpu.VMEM((4 * kvec, 256), F32),
            pltpu.VMEM((8, kvec, 128), F32),
            pltpu.VMEM((LOW, kvec, 128), F32),
            pltpu.VMEM((n_high, kvec, 128), F32),
            pltpu.VMEM((8, kvec, 128), F32),
            dma((STAGES,)), dma((3,)), dma,
            dma((ITERS + 1,)), dma((ITERS + 1,)), dma((ITERS + 1,)), dma((ITERS + 1,)),
            dma((ITERS, LOW)), dma((ITERS, LOW)), dma((ITERS, n_high)), dma((ITERS, n_high)),
            dma((LOW,)), dma((LOW,)), dma((n_high,)), dma((n_high,)), dma((LOW,)), dma((LOW,)),
        ],
        compiler_params=pltpu.CompilerParams(
            collective_id=0, has_side_effects=True, vmem_limit_bytes=60 * 1024 * 1024
        ),
    )(block_cols, live_counts, blocks, onsite_energy.reshape(rows, 1, bs), precond, vectors, prev_vectors, prev_image)
    gram = mats[0:4].reshape(4 * kvec, 128)
    proj = mats[4:8].reshape(4 * kvec, 128)
    step = gram[0:kvec, 96] / (gram[0:kvec, 97] + 1.0)

    def combine(x):
        x = jnp.concatenate([x[0:64], x[64:96] + step[:, None] * x[96:128]], axis=0)
        return jnp.concatenate([x[:, 0:64], x[:, 64:96] + step[None, :] * x[:, 96:128]], axis=1)

    lower = combine(gram)
    tail = lower[64:96]
    gram_matrix = jnp.concatenate(
        [jnp.concatenate([lower[0:64, 0:64], tail[:, 0:64].T], axis=1), tail], axis=0
    )
    projected = combine(proj)
    gram_matrix = gram_matrix + jnp.eye(gram_matrix.shape[0], dtype=F32)
    factor = jnp.linalg.cholesky(gram_matrix)
    half_way = jax.scipy.linalg.solve_triangular(factor, projected, lower=True)
    reduced = jax.scipy.linalg.solve_triangular(factor, half_way.T, lower=True).T
    return correction, reduced


def solution(mesh):
    n_dev = mesh.shape["rows"]

    def step(*args):
        return local(n_dev, *args)

    return jax.shard_map(
        step,
        mesh=mesh,
        in_specs=(
            P("rows", None, None, None), P("rows", None), P("rows"), P("rows"),
            P("rows", None, None), P(None, "rows"), P(None, "rows"), P(None, "rows"),
        ),
        out_specs=(P(None, "rows"), P()),
        check_vma=False,
    )
```

```python
import jax
import jax.numpy as jnp
from jax import lax
from jax.experimental import pallas as pl
from jax.experimental.pallas import tpu as pltpu
from jax.sharding import PartitionSpec as P

MESH = pl.DeviceIdType.MESH
F32 = jnp.float32
BF16 = jnp.bfloat16
HB = 4
ITERS = 3
LOW = 8
SLOTS = 4
STAGES = 4


def split(x):
    high = x.astype(BF16)
    return high, (x - high.astype(F32)).astype(BF16)


def mm(a, b):
    return jnp.dot(a, b, preferred_element_type=F32)


def mmt(a, b):
    return lax.dot_general(a, b, (((1,), (1,)), ((), ())), preferred_element_type=F32)


def reduce_basis(gram, proj, step, aug, kvec):
    width = 128
    size = 3 * kvec
    lane = lax.broadcasted_iota(jnp.int32, (kvec, width), 1)
    row = lax.broadcasted_iota(jnp.int32, (kvec, width), 0)
    step_row = jnp.sum(jnp.where(lane == row + size, step, 0.0), axis=0, keepdims=True)

    def fold(x):
        n = x.shape[0]
        at = lax.broadcasted_iota(jnp.int32, (n, width), 1)
        moved = pltpu.roll(x * step_row, width - kvec, 1)
        return jnp.where(at < 2 * kvec, x, jnp.where(at < size, x + moved, 0.0))

    tail = fold(gram[2] + step * gram[3])
    above = jnp.concatenate([jnp.zeros((2 * kvec, width), F32), tail, jnp.zeros((kvec, width), F32)], axis=0).T
    for g in range(2):
        a = jnp.where(lane < 2 * kvec, gram[g], above[g * kvec:(g + 1) * kvec])
        aug[g * kvec:(g + 1) * kvec, 0:width] = a + jnp.where(lane == row + g * kvec, 1.0, 0.0)
    aug[2 * kvec:size, 0:width] = tail + jnp.where(lane == row + 2 * kvec, 1.0, 0.0)
    for g in range(3):
        aug[g * kvec:(g + 1) * kvec, width:2 * width] = jnp.where(lane == row + g * kvec, 1.0, 0.0)
    x = jnp.concatenate([fold(proj[0]), fold(proj[1]), fold(proj[2] + step * proj[3]), jnp.zeros((kvec, width), F32)], axis=0)

    sub = lax.broadcasted_iota(jnp.int32, (8, width), 0)
    for top in range(0, size, 8):
        n = size - top
        cols = [jnp.broadcast_to(aug[top:size, top + c:top + c + 1], (n, width)) for c in range(8)]
        pivot_rows = aug[top:top + 8, :]
        facs = []
        for j in range(8):
            f = cols[j] * (1.0 / cols[j][j:j + 1, :])
            head = jnp.where(sub > j, f[0:8], 0.0)
            facs.append(f)
            for c in range(j + 1, 8):
                pr = cols[c][j:j + 1, :]
                new_head = cols[c][0:8] - head * pr
                cols[c] = new_head if n == 8 else jnp.concatenate([new_head, cols[c][8:] - f[8:] * pr], axis=0)
            both = jnp.concatenate([head, head], axis=1)
            pivot_rows = pivot_rows - both * pivot_rows[j:j + 1, :]
        aug[top:top + 8, :] = pivot_rows
        for r in range(top + 8, size, 8):
            block = aug[r:r + 8, :]
            for j in range(8):
                f = facs[j][r - top:r - top + 8]
                block = block - jnp.concatenate([f, f], axis=1) * pivot_rows[j:j + 1, :]
            aug[r:r + 8, :] = block

    at = lax.broadcasted_iota(jnp.int32, (size, width), 1)
    diagonal = jnp.where(at == lax.broadcasted_iota(jnp.int32, (size, width), 0), aug[:, 0:width], 0.0)
    by_row = lax.rsqrt(jnp.sum(diagonal, axis=1, keepdims=True))
    by_col = jnp.sum(diagonal, axis=0, keepdims=True)
    by_col = jnp.where(at[0:1] < size, lax.rsqrt(jnp.where(at[0:1] < size, by_col, 1.0)), 0.0)
    w = aug[:, width:2 * width]
    w_full = jnp.concatenate([w, jnp.zeros((kvec, width), F32)], axis=0)
    half = jnp.dot(w, x, precision=lax.Precision.HIGHEST, preferred_element_type=F32)
    full = lax.dot_general(half, w_full, (((1,), (1,)), ((), ())), precision=lax.Precision.HIGHEST, preferred_element_type=F32)
    return full * by_row * by_col


def kernel(
    n_dev, rows, kvec, bs,
    cols, live, blocks, onsite, precond, vec, pvec, pimg,
    corr, mats,
    stage, bh, bl, ph, plo, offs,
    fv, fpv, fpi, fim, fr, fu, fhu, fa, fz, fc, fh, zs, acc, qb, sb,
    zhalo, inc, spill, red1, red2, gram, parts, big1, big2, fin, aug,
    stage_sem, load_sem, out_sem, zs_sem, zr_sem, ss_sem, sr_sem,
    r1s, r1r, r2s, r2r, b1s, b1r, b2s, b2r, b3s, b3r,
):
    me = lax.axis_index("rows")
    low = lax.rem(me, LOW)
    high = lax.div(me, LOW)
    n_high = n_dev // LOW
    total = n_dev * rows
    first = me * rows
    right = lax.rem(me + 1, n_dev)
    left = lax.rem(me + n_dev - 1, n_dev)
    edge = rows - HB
    order = list(range(edge, rows)) + list(range(edge))

    def load_field(src, dst, sem):
        for b in range(rows):
            pltpu.make_async_copy(src.at[:, pl.ds(b * bs, bs)], dst.at[b], sem).start()

    def load_wait(dst, sem):
        pltpu.make_async_copy(dst, dst, sem).wait()

    n_chunks = rows + rows // SLOTS

    def chunk(i):
        slot = i % STAGES
        if i < rows:
            src = blocks.at[order[i]]
        else:
            src = precond.at[pl.ds((i - rows) * SLOTS, SLOTS)]
        return pltpu.make_async_copy(src, stage.at[slot], stage_sem.at[slot])

    load_field(vec, fv, load_sem.at[0])
    for i in range(STAGES):
        chunk(i).start()

    barrier = pltpu.get_barrier_semaphore()
    peers = [left, right]
    peers += [high * LOW + lax.rem(low + j, LOW) for j in range(1, LOW)]
    peers += [lax.rem(high + j, n_high) * LOW + low for j in range(1, n_high)]
    for peer in peers:
        pl.semaphore_signal(barrier, inc=1, device_id=(peer,), device_id_type=MESH)
    pl.semaphore_wait(barrier, len(peers))

    def rcopy(src, dst, s_sem, r_sem, to):
        return pltpu.make_async_remote_copy(
            src_ref=src, dst_ref=dst, send_sem=s_sem, recv_sem=r_sem,
            device_id=(to,), device_id_type=MESH,
        )

    def z_copy(n, field):
        return rcopy(field.at[pl.ds(0, HB)], zhalo.at[n], zs_sem.at[n], zr_sem.at[n], left)

    def spill_copy(n):
        return rcopy(spill.at[n], inc.at[n], ss_sem.at[n], sr_sem.at[n], right)

    def low_copy(i, j):
        to = high * LOW + lax.rem(low + j, LOW)
        return rcopy(red1.at[i, low], red1.at[i, low], r1s.at[i, j], r1r.at[i, low], to)

    def low_in(i, j):
        frm = lax.rem(low + j, LOW)
        return rcopy(red1.at[i, frm], red1.at[i, frm], r1s.at[i, j], r1r.at[i, frm], left)

    def high_copy(i, j):
        to = lax.rem(high + j, n_high) * LOW + low
        return rcopy(red2.at[i, high], red2.at[i, high], r2s.at[i, j], r2r.at[i, high], to)

    def high_in(i, j):
        frm = lax.rem(high + j, n_high)
        return rcopy(red2.at[i, frm], red2.at[i, frm], r2s.at[i, j], r2r.at[i, frm], left)

    lane = lax.broadcasted_iota(jnp.int32, (8, 128), 1)
    groups = kvec // 8

    def pack(a, b):
        tile = jnp.zeros((8, 128), F32)
        for g in range(groups):
            tile = tile + jnp.where(lane == g, a[8 * g:8 * g + 8], 0.0)
            tile = tile + jnp.where(lane == groups + g, b[8 * g:8 * g + 8], 0.0)
        return tile

    def unpack(tile):
        out = []
        for base in (0, groups):
            out.append(jnp.concatenate(
                [jnp.sum(jnp.where(lane == base + g, tile, 0.0), axis=1, keepdims=True) for g in range(groups)],
                axis=0,
            ))
        return out

    def red_start(i, a, b):
        red1[i, low] = pack(a, b)
        for j in range(1, LOW):
            low_copy(i, j).start()

    def red_mid(i):
        for j in range(1, LOW):
            low_in(i, j).wait_recv()
        tile = red1[i, 0]
        for l in range(1, LOW):
            tile = tile + red1[i, l]
        red2[i, high] = tile
        for j in range(1, n_high):
            high_copy(i, j).start()

    def red_end(i):
        for j in range(1, n_high):
            high_in(i, j).wait_recv()
        tile = red2[i, 0]
        for l in range(1, n_high):
            tile = tile + red2[i, l]
        for j in range(1, LOW):
            low_copy(i, j).wait_send()
        for j in range(1, n_high):
            high_copy(i, j).wait_send()
        return unpack(tile)

    def put_split(b, z):
        zh, zl = split(z)
        zs[b, 0:kvec, :] = zh
        zs[b, kvec:2 * kvec, :] = zl

    def onto(b):
        zb = zs[b]
        zh = zb[0:kvec]
        sums = [None] * (HB + 1)
        for s in range(SLOTS):
            part = mm(zb, bh[b * SLOTS + s])
            moved = part[0:kvec] + part[kvec:] + mm(zh, bl[b * SLOTS + s])
            off = offs[b * SLOTS + s]
            for o in range(HB + 1):
                term = jnp.where(off == o, 1.0, 0.0) * moved
                sums[o] = term if sums[o] is None else sums[o] + term
        for o in range(HB + 1):
            acc[b + o] = acc[b + o] + sums[o]

    def across(b):
        out = None
        for s in range(SLOTS):
            zc = zs[b + offs[b * SLOTS + s]]
            part = mmt(zc, bh[b * SLOTS + s])
            term = part[0:kvec] + part[kvec:] + mmt(zc[0:kvec], bl[b * SLOTS + s])
            out = term if out is None else out + term
        acc[b] = acc[b] + out

    def halo_in(n):
        z_copy(n, fv).wait_recv()
        for t in range(HB):
            put_split(rows + t, zhalo[n, t])

    def send_spill(n):
        for t in range(HB):
            spill[n, t] = acc[rows + t]
        spill_copy(n).start()

    def take_in(n):
        spill_copy(n).wait_recv()
        for t in range(HB):
            acc[t] = acc[t] + inc[n, t]

    def diag(b, z):
        acc[b] = onsite[b] * z

    def clear_tail():
        for t in range(HB):
            acc[rows + t] = jnp.zeros((kvec, bs), F32)

    load_wait(fv, load_sem.at[0])
    z_copy(0, fv).start()
    load_field(pvec, fpv, load_sem.at[1])
    load_field(pimg, fpi, load_sem.at[2])

    def prepare(b, c):
        z = fv[b]
        put_split(b, z)
        diag(b, z)
        return c

    lax.fori_loop(0, rows, prepare, 0)
    clear_tail()

    def take_chunk(i):
        chunk(i).wait()
        slot = i % STAGES
        if i < rows:
            b = order[i]
            for s in range(SLOTS):
                off = lax.rem(cols[b, s] - first - b + 2 * total, total)
                offs[b * SLOTS + s] = jnp.minimum(off, HB)
                alive = jnp.where(s < live[b], 1.0, 0.0)

                def piece(p, c):
                    at = pl.ds(pl.multiple_of(p * 64, 64), 64)
                    xh, xl = split(stage[slot, s, at, :] * alive)
                    bh[b * SLOTS + s, at, :] = xh
                    bl[b * SLOTS + s, at, :] = xl
                    return c

                lax.fori_loop(0, bs // 64, piece, 0)
        else:
            for s in range(SLOTS):
                def piece(p, c):
                    at = pl.ds(pl.multiple_of(p * 64, 64), 64)
                    xh, xl = split(stage[slot, s, at, :])
                    ph[(i - rows) * SLOTS + s, at, :] = xh
                    plo[(i - rows) * SLOTS + s, at, :] = xl
                    return c

                lax.fori_loop(0, bs // 64, piece, 0)
        if i + STAGES < n_chunks:
            chunk(i + STAGES).start()

    for i in range(HB):
        take_chunk(i)
        onto(order[i])
    send_spill(0)
    for i in range(HB, rows):
        take_chunk(i)
        onto(order[i])
        across(order[i])
    halo_in(0)
    for b in range(edge, rows):
        across(b)
    take_in(0)

    zero = jnp.zeros((kvec, bs), F32)

    def first_sums(b, c):
        x, im = fv[b], acc[b]
        fim[b] = im
        return c[0] + x * im, c[1] + x * x

    num, den = lax.fori_loop(0, rows, first_sums, (zero, zero))
    total_of = lambda x: jnp.sum(x, axis=1, keepdims=True)
    red_start(0, total_of(num), total_of(den))
    for i in range(rows, n_chunks):
        take_chunk(i)
    red_mid(0)
    num, den = red_end(0)
    q = num / den
    qb[...] = jnp.broadcast_to(q, (kvec, bs))

    def first_rest(b, c):
        fr[b] = qb[...] * fv[b] - fim[b]
        return c

    lax.fori_loop(0, rows, first_rest, 0)

    def precondition(field, b):
        dh, dl = split(field[b])
        both = jnp.concatenate([dh, dl], axis=0)
        part = mmt(both, ph[b])
        z = part[0:kvec] + part[kvec:] + mmt(dh, plo[b])
        fz[b] = z
        put_split(b, z)
        diag(b, z)

    for k in range(ITERS):
        n = k + 1
        field = fr if k == 0 else fa
        for b in range(HB):
            precondition(field, b)
        z_copy(n, fz).start()
        clear_tail()
        for b in range(edge, rows):
            precondition(field, b)
        for b in range(edge, rows):
            onto(b)
        send_spill(n)

        def interior(g, c, field=field):
            for t in range(4):
                precondition(field, 4 + 4 * g + t)
            return c

        lax.fori_loop(0, (edge - HB) // 4, interior, 0)
        if k > 0:
            red_mid(k)

        def body(g, c):
            for t in range(4):
                onto(4 * g + t)
            for t in range(4):
                across(4 * g + t)
            return c

        lax.fori_loop(0, edge // 4, body, 0)
        halo_in(n)
        for b in range(edge, rows):
            across(b)
        take_in(n)
        z_copy(n, fz).wait_send()
        if k > 0:
            cross, own = red_end(k)
            step = cross / (own + 1.0)
            sb[...] = jnp.broadcast_to(step, (kvec, bs))

        def update(b, c, k=k):
            z, hz = fz[b], acc[b]
            m = hz - qb[...] * z
            if k == 0:
                r = fr[b]
                a = m
                fu[b] = z
                fhu[b] = hz
            else:
                s = sb[...]
                u, hu, a = fu[b], fhu[b], fa[b]
                r = fr[b] - s * a
                fr[b] = r
                if k == 1:
                    fc[b] = s * u
                    fh[b] = s * hu
                else:
                    fc[b] = fc[b] + s * u
                    fh[b] = fh[b] + s * hu
                a = a - s * m
                fu[b] = u - s * z
                fhu[b] = hu - s * hz
            fa[b] = a
            return c[0] + a * r, c[1] + a * a

        cross, own = lax.fori_loop(0, rows, update, (zero, zero))
        if k + 1 < ITERS:
            red_start(k + 1, total_of(cross), total_of(own))

    load_wait(fpv, load_sem.at[1])
    load_wait(fpi, load_sem.at[2])
    gram[...] = jnp.zeros_like(gram)

    def products(b, c):
        xh, xl = split(jnp.concatenate([fv[b], fpv[b], fc[b], fu[b]], axis=0))
        yh, yl = split(jnp.concatenate([fim[b], fpi[b], fh[b], fhu[b]], axis=0))
        part = mmt(jnp.concatenate([xh, xl], axis=0), jnp.concatenate([xh, yh], axis=0))
        m = xh.shape[0]
        gram[...] = gram[...] + (part[0:m] + part[m:] + mmt(xh, jnp.concatenate([xl, yl], axis=0)))
        return c

    lax.fori_loop(0, rows, products, 0)
    wide = lax.broadcasted_iota(jnp.int32, (kvec, 128), 1)
    for p in range(4):
        at = pl.ds(p * kvec, kvec)
        g = gram[at, 0:128]
        if p == 0:
            g = jnp.where(wide == 96, total_of(cross), jnp.where(wide == 97, total_of(own), g))
        parts[p] = g
        parts[4 + p] = gram[at, 128:256]

    def big1_copy(j):
        to = lax.rem(low + j, LOW)
        return rcopy(parts.at[to], big1.at[low], b1s.at[j], b1r.at[low], high * LOW + to)

    def big1_in(j):
        frm = lax.rem(low + j, LOW)
        return rcopy(parts.at[frm], big1.at[frm], b1s.at[j], b1r.at[frm], left)

    def big2_copy(j):
        to = lax.rem(high + j, n_high) * LOW + low
        return rcopy(big2.at[high], big2.at[high], b2s.at[j], b2r.at[high], to)

    def big2_in(j):
        frm = lax.rem(high + j, n_high)
        return rcopy(big2.at[frm], big2.at[frm], b2s.at[j], b2r.at[frm], left)

    def fin_copy(j):
        to = high * LOW + lax.rem(low + j, LOW)
        return rcopy(fin.at[low], fin.at[low], b3s.at[j], b3r.at[low], to)

    def fin_in(j):
        frm = lax.rem(low + j, LOW)
        return rcopy(fin.at[frm], fin.at[frm], b3s.at[j], b3r.at[frm], left)

    for j in range(1, LOW):
        big1_copy(j).start()
    big1[low] = parts[low]
    for j in range(1, LOW):
        big1_in(j).wait_recv()
    tile = big1[0]
    for l in range(1, LOW):
        tile = tile + big1[l]
    big2[high] = tile
    for j in range(1, n_high):
        big2_copy(j).start()
    for j in range(1, n_high):
        big2_in(j).wait_recv()
    tile = big2[0]
    for l in range(1, n_high):
        tile = tile + big2[l]
    fin[low] = tile
    for j in range(1, LOW):
        fin_copy(j).start()
    for j in range(1, LOW):
        fin_in(j).wait_recv()

    head = fin[0]
    step = head[:, 96:97] / (head[:, 97:98] + 1.0)
    sb[...] = jnp.broadcast_to(step, (kvec, bs))

    def finish(b, c):
        fc[b] = fc[b] + sb[...] * fu[b]
        return c

    lax.fori_loop(0, rows, finish, 0)
    for b in range(rows):
        pltpu.make_async_copy(fc.at[b], corr.at[:, pl.ds(b * bs, bs)], out_sem).start()
    mats[...] = reduce_basis([fin[p] for p in range(4)], [fin[p] for p in range(4, 8)], step, aug, kvec)
    pltpu.make_async_copy(fc, fc, out_sem).wait()

    for j in range(1, LOW):
        big1_copy(j).wait_send()
        fin_copy(j).wait_send()
    for j in range(1, n_high):
        big2_copy(j).wait_send()
    z_copy(0, fv).wait_send()
    for n in range(ITERS + 1):
        spill_copy(n).wait_send()


def local(n_dev, blocks, block_cols, live_counts, onsite_energy, precond, vectors, prev_vectors, prev_image):
    rows, slots, bs = blocks.shape[0], blocks.shape[1], blocks.shape[2]
    kvec = vectors.shape[0]
    n_high = n_dev // LOW
    field = pltpu.VMEM((rows, kvec, bs), F32)
    dma = pltpu.SemaphoreType.DMA
    hbm = pl.BlockSpec(memory_space=pl.ANY)
    smem = pl.BlockSpec(memory_space=pltpu.SMEM)
    vmem = pl.BlockSpec(memory_space=pltpu.VMEM)

    def run(*args):
        return kernel(n_dev, rows, kvec, bs, *args)

    correction, mats = pl.pallas_call(
        run,
        out_shape=(
            jax.ShapeDtypeStruct(vectors.shape, F32),
            jax.ShapeDtypeStruct((3 * kvec, 128), F32),
        ),
        in_specs=[smem, smem, hbm, vmem, hbm, hbm, hbm, hbm],
        out_specs=(hbm, vmem),
        scratch_shapes=[
            pltpu.VMEM((STAGES, slots, bs, bs), F32),
            pltpu.VMEM((rows * slots, bs, bs), BF16),
            pltpu.VMEM((rows * slots, bs, bs), BF16),
            pltpu.VMEM((rows, bs, bs), BF16),
            pltpu.VMEM((rows, bs, bs), BF16),
            pltpu.SMEM((rows * slots,), jnp.int32),
            field, field, field, field, field, field, field, field, field, field, field,
            pltpu.VMEM((rows + HB, 2 * kvec, bs), BF16),
            pltpu.VMEM((rows + HB, kvec, bs), F32),
            pltpu.VMEM((kvec, bs), F32),
            pltpu.VMEM((kvec, bs), F32),
            pltpu.VMEM((ITERS + 1, HB, kvec, bs), F32),
            pltpu.VMEM((ITERS + 1, HB, kvec, bs), F32),
            pltpu.VMEM((ITERS + 1, HB, kvec, bs), F32),
            pltpu.VMEM((ITERS, LOW, 8, 128), F32),
            pltpu.VMEM((ITERS, n_high, 8, 128), F32),
            pltpu.VMEM((4 * kvec, 256), F32),
            pltpu.VMEM((8, kvec, 128), F32),
            pltpu.VMEM((LOW, kvec, 128), F32),
            pltpu.VMEM((n_high, kvec, 128), F32),
            pltpu.VMEM((8, kvec, 128), F32),
            pltpu.VMEM((3 * kvec, 256), F32),
            dma((STAGES,)), dma((3,)), dma,
            dma((ITERS + 1,)), dma((ITERS + 1,)), dma((ITERS + 1,)), dma((ITERS + 1,)),
            dma((ITERS, LOW)), dma((ITERS, LOW)), dma((ITERS, n_high)), dma((ITERS, n_high)),
            dma((LOW,)), dma((LOW,)), dma((n_high,)), dma((n_high,)), dma((LOW,)), dma((LOW,)),
        ],
        compiler_params=pltpu.CompilerParams(
            collective_id=0, has_side_effects=True, vmem_limit_bytes=60 * 1024 * 1024
        ),
    )(block_cols, live_counts, blocks, onsite_energy.reshape(rows, 1, bs), precond, vectors, prev_vectors, prev_image)
    return correction, mats[:, 0:3 * kvec]


def solution(mesh):
    n_dev = mesh.shape["rows"]

    def step(*args):
        return local(n_dev, *args)

    return jax.shard_map(
        step,
        mesh=mesh,
        in_specs=(
            P("rows", None, None, None), P("rows", None), P("rows"), P("rows"),
            P("rows", None, None), P(None, "rows"), P(None, "rows"), P(None, "rows"),
        ),
        out_specs=(P(None, "rows"), P()),
        check_vma=False,
    )
```

```python
import jax
import jax.numpy as jnp
from jax import lax
from jax.experimental import pallas as pl
from jax.experimental.pallas import tpu as pltpu
from jax.sharding import PartitionSpec as P

MESH = pl.DeviceIdType.MESH
F32 = jnp.float32
BF16 = jnp.bfloat16
HB = 4
ITERS = 3
LOW = 8
SLOTS = 4
STAGES = 4


def split(x):
    high = x.astype(BF16)
    return high, (x - high.astype(F32)).astype(BF16)


def mm(a, b):
    return jnp.dot(a, b, preferred_element_type=F32)


def mmt(a, b):
    return lax.dot_general(a, b, (((1,), (1,)), ((), ())), preferred_element_type=F32)


def reduce_basis(gram, proj, step, aug, kvec):
    width = 128
    size = 3 * kvec
    lane = lax.broadcasted_iota(jnp.int32, (kvec, width), 1)
    row = lax.broadcasted_iota(jnp.int32, (kvec, width), 0)
    step_row = jnp.sum(jnp.where(lane == row + size, step, 0.0), axis=0, keepdims=True)

    def fold(x):
        n = x.shape[0]
        at = lax.broadcasted_iota(jnp.int32, (n, width), 1)
        moved = pltpu.roll(x * step_row, width - kvec, 1)
        return jnp.where(at < 2 * kvec, x, jnp.where(at < size, x + moved, 0.0))

    tail = fold(gram[2] + step * gram[3])
    above = jnp.concatenate([jnp.zeros((2 * kvec, width), F32), tail, jnp.zeros((kvec, width), F32)], axis=0).T
    for g in range(2):
        a = jnp.where(lane < 2 * kvec, gram[g], above[g * kvec:(g + 1) * kvec])
        aug[g * kvec:(g + 1) * kvec, 0:width] = a + jnp.where(lane == row + g * kvec, 1.0, 0.0)
    aug[2 * kvec:size, 0:width] = tail + jnp.where(lane == row + 2 * kvec, 1.0, 0.0)
    for g in range(3):
        aug[g * kvec:(g + 1) * kvec, width:2 * width] = jnp.where(lane == row + g * kvec, 1.0, 0.0)
    x = jnp.concatenate([fold(proj[0]), fold(proj[1]), fold(proj[2] + step * proj[3]), jnp.zeros((kvec, width), F32)], axis=0)

    sub = lax.broadcasted_iota(jnp.int32, (8, width), 0)
    for top in range(0, size, 8):
        n = size - top
        cols = [jnp.broadcast_to(aug[top:size, top + c:top + c + 1], (n, width)) for c in range(8)]
        pivot_rows = aug[top:top + 8, :]
        facs = []
        for j in range(8):
            f = cols[j] * (1.0 / cols[j][j:j + 1, :])
            head = jnp.where(sub > j, f[0:8], 0.0)
            facs.append(f)
            for c in range(j + 1, 8):
                pr = cols[c][j:j + 1, :]
                new_head = cols[c][0:8] - head * pr
                cols[c] = new_head if n == 8 else jnp.concatenate([new_head, cols[c][8:] - f[8:] * pr], axis=0)
            both = jnp.concatenate([head, head], axis=1)
            pivot_rows = pivot_rows - both * pivot_rows[j:j + 1, :]
        aug[top:top + 8, :] = pivot_rows
        for r in range(top + 8, size, 8):
            block = aug[r:r + 8, :]
            for j in range(8):
                f = facs[j][r - top:r - top + 8]
                block = block - jnp.concatenate([f, f], axis=1) * pivot_rows[j:j + 1, :]
            aug[r:r + 8, :] = block

    at = lax.broadcasted_iota(jnp.int32, (size, width), 1)
    diagonal = jnp.where(at == lax.broadcasted_iota(jnp.int32, (size, width), 0), aug[:, 0:width], 0.0)
    by_row = lax.rsqrt(jnp.sum(diagonal, axis=1, keepdims=True))
    by_col = jnp.sum(diagonal, axis=0, keepdims=True)
    by_col = jnp.where(at[0:1] < size, lax.rsqrt(jnp.where(at[0:1] < size, by_col, 1.0)), 0.0)
    w = aug[:, width:2 * width]
    w_full = jnp.concatenate([w, jnp.zeros((kvec, width), F32)], axis=0)
    half = jnp.dot(w, x, precision=lax.Precision.HIGHEST, preferred_element_type=F32)
    full = lax.dot_general(half, w_full, (((1,), (1,)), ((), ())), precision=lax.Precision.HIGHEST, preferred_element_type=F32)
    return full * by_row * by_col


def kernel(
    n_dev, rows, kvec, bs,
    cols, live, blocks, onsite, precond, vec, pvec, pimg,
    c_out, u_out, mats,
    stage, bh, bl, th, tl, ph, plo, offs,
    fw, fhw, fpv, fpi, fim, fr, fu, fhu, fa, fz, fc, fh, zsw, accw, zs, acc, qb, sb,
    zhalo, inc, spill, zhalo0, inc0, spill0, red1, red2, gram, parts, big1, big2, fin,
    stage_sem, load_sem, out_sem, zs_sem, zr_sem, ss_sem, sr_sem,
    r1s, r1r, r2s, r2r, b1s, b1r, b2s, b2r, b3s, b3r,
):
    me = lax.axis_index("rows")
    low = lax.rem(me, LOW)
    high = lax.div(me, LOW)
    n_high = n_dev // LOW
    total = n_dev * rows
    first = me * rows
    right = lax.rem(me + 1, n_dev)
    left = lax.rem(me + n_dev - 1, n_dev)
    edge = rows - HB

    def field_copy(hbm, b):
        return hbm.at[:, pl.ds(b * bs, bs)]

    def block_copy(row, slot):
        return pltpu.make_async_copy(blocks.at[row], stage.at[slot], stage_sem.at[slot])

    def precond_copy(j):
        return pltpu.make_async_copy(precond.at[pl.ds(j * SLOTS, SLOTS)], stage.at[j], stage_sem.at[j])

    def start_loads(b, c):
        at = pl.ds(pl.multiple_of(b * bs, bs), bs)
        pltpu.make_async_copy(vec.at[:, at], fw.at[b, pl.ds(0, kvec)], load_sem.at[0]).start()
        return c

    lax.fori_loop(0, rows, start_loads, 0)
    for j in range(STAGES):
        precond_copy(j).start()

    def start_more(b, c):
        at = pl.ds(pl.multiple_of(b * bs, bs), bs)
        pltpu.make_async_copy(pvec.at[:, at], fpv.at[b], load_sem.at[1]).start()
        pltpu.make_async_copy(pimg.at[:, at], fpi.at[b], load_sem.at[2]).start()
        return c

    barrier = pltpu.get_barrier_semaphore()
    peers = [left, right]
    peers += [high * LOW + lax.rem(low + j, LOW) for j in range(1, LOW)]
    peers += [lax.rem(high + j, n_high) * LOW + low for j in range(1, n_high)]
    for peer in peers:
        pl.semaphore_signal(barrier, inc=1, device_id=(peer,), device_id_type=MESH)

    def rcopy(src, dst, s_sem, r_sem, to):
        return pltpu.make_async_remote_copy(
            src_ref=src, dst_ref=dst, send_sem=s_sem, recv_sem=r_sem,
            device_id=(to,), device_id_type=MESH,
        )

    def z_copy(n):
        src, dst = (fw, zhalo0) if n == 0 else (fz, zhalo.at[n - 1])
        return rcopy(src.at[pl.ds(0, HB)], dst, zs_sem.at[n], zr_sem.at[n], left)

    def spill_copy(n):
        src, dst = (spill0, inc0) if n == 0 else (spill.at[n - 1], inc.at[n - 1])
        return rcopy(src, dst, ss_sem.at[n], sr_sem.at[n], right)

    def low_copy(i, j):
        to = high * LOW + lax.rem(low + j, LOW)
        return rcopy(red1.at[i, low], red1.at[i, low], r1s.at[i, j], r1r.at[i, low], to)

    def low_in(i, j):
        frm = lax.rem(low + j, LOW)
        return rcopy(red1.at[i, frm], red1.at[i, frm], r1s.at[i, j], r1r.at[i, frm], left)

    def high_copy(i, j):
        to = lax.rem(high + j, n_high) * LOW + low
        return rcopy(red2.at[i, high], red2.at[i, high], r2s.at[i, j], r2r.at[i, high], to)

    def high_in(i, j):
        frm = lax.rem(high + j, n_high)
        return rcopy(red2.at[i, frm], red2.at[i, frm], r2s.at[i, j], r2r.at[i, frm], left)

    lane = lax.broadcasted_iota(jnp.int32, (8, 128), 1)
    groups = kvec // 8

    def pack(a, b):
        tile = jnp.zeros((8, 128), F32)
        for g in range(groups):
            tile = tile + jnp.where(lane == g, a[8 * g:8 * g + 8], 0.0)
            tile = tile + jnp.where(lane == groups + g, b[8 * g:8 * g + 8], 0.0)
        return tile

    def unpack(tile):
        out = []
        for base in (0, groups):
            out.append(jnp.concatenate(
                [jnp.sum(jnp.where(lane == base + g, tile, 0.0), axis=1, keepdims=True) for g in range(groups)],
                axis=0,
            ))
        return out

    def red_start(i, a, b):
        red1[i, low] = pack(a, b)
        for j in range(1, LOW):
            low_copy(i, j).start()

    def red_mid(i):
        for j in range(1, LOW):
            low_in(i, j).wait_recv()
        tile = red1[i, 0]
        for l in range(1, LOW):
            tile = tile + red1[i, l]
        red2[i, high] = tile
        for j in range(1, n_high):
            high_copy(i, j).start()

    def red_end(i):
        for j in range(1, n_high):
            high_in(i, j).wait_recv()
        tile = red2[i, 0]
        for l in range(1, n_high):
            tile = tile + red2[i, l]
        for j in range(1, LOW):
            low_copy(i, j).wait_send()
        for j in range(1, n_high):
            high_copy(i, j).wait_send()
        return unpack(tile)

    class Apply:
        def __init__(self, kv, parts_ref, acc_ref):
            self.kv, self.zs, self.acc = kv, parts_ref, acc_ref

        def put(self, b, z):
            zh, zl = split(z)
            self.zs[b, 0:self.kv, :] = zh
            self.zs[b, self.kv:2 * self.kv, :] = zl

        def diag(self, b, z):
            self.acc[b] = onsite[b] * z

        def clear_tail(self):
            for t in range(HB):
                self.acc[rows + t] = jnp.zeros((self.kv, bs), F32)

        def product(self, z, hi, lo):
            part = mm(z, hi)
            return part[0:self.kv] + part[self.kv:] + mm(z[0:self.kv], lo)

        def onto(self, b):
            zb = self.zs[b]
            sums = [None] * (HB + 1)
            for s in range(SLOTS):
                moved = self.product(zb, bh[b * SLOTS + s], bl[b * SLOTS + s])
                off = offs[b * SLOTS + s]
                for o in range(HB + 1):
                    term = jnp.where(off == o, 1.0, 0.0) * moved
                    sums[o] = term if sums[o] is None else sums[o] + term
            for o in range(HB + 1):
                self.acc[b + o] = self.acc[b + o] + sums[o]

        def across(self, b):
            out = None
            for s in range(SLOTS):
                term = self.product(self.zs[b + offs[b * SLOTS + s]], th[b * SLOTS + s], tl[b * SLOTS + s])
                out = term if out is None else out + term
            self.acc[b] = self.acc[b] + out

        def halo_in(self, n):
            z_copy(n).wait_recv()
            for t in range(HB):
                self.put(rows + t, zhalo0[t] if n == 0 else zhalo[n - 1, t])

        def send_spill(self, n):
            for t in range(HB):
                if n == 0:
                    spill0[t] = self.acc[rows + t]
                else:
                    spill[n - 1, t] = self.acc[rows + t]
            spill_copy(n).start()

        def take_in(self, n):
            spill_copy(n).wait_recv()
            for t in range(HB):
                self.acc[t] = self.acc[t] + (inc0[t] if n == 0 else inc[n - 1, t])

    wide = Apply(2 * kvec, zsw, accw)
    thin = Apply(kvec, zs, acc)

    def precondition(x, b):
        dh, dl = split(x)
        part = mm(jnp.concatenate([dh, dl], axis=0), ph[b])
        return part[0:kvec] + part[kvec:] + mm(dh, plo[b])

    pltpu.make_async_copy(fw.at[:, pl.ds(0, kvec)], fw.at[:, pl.ds(0, kvec)], load_sem.at[0]).wait()
    for j in range(rows // SLOTS):
        precond_copy(j).wait()
        for t in range(SLOTS):
            b = j * SLOTS + t
            xh, xl = split(stage[j, t])
            ph[b] = xh.T
            plo[b] = xl.T
        block_copy(edge + j, j).start()
        for t in range(SLOTS):
            b = j * SLOTS + t
            v = fw[b, 0:kvec]
            fw[b, kvec:2 * kvec] = precondition(v, b)
            x = fw[b]
            wide.put(b, x)
            wide.diag(b, x)
        if j == 0:
            pl.semaphore_wait(barrier, len(peers))
            z_copy(0).start()
    lax.fori_loop(0, rows, start_more, 0)
    wide.clear_tail()

    def take_row(b, slot):
        block_copy(b, slot).wait()
        for s in range(SLOTS):
            off = cols[s, b] - first - b
            off = jnp.where(off < 0, off + total, off)
            offs[b * SLOTS + s] = jnp.minimum(off, HB)
            alive = jnp.where(s < live[b], 1.0, 0.0)
            xh, xl = split(stage[slot, s] * alive)
            bh[b * SLOTS + s] = xh
            bl[b * SLOTS + s] = xl
            th[b * SLOTS + s] = xh.T
            tl[b * SLOTS + s] = xl.T

    def tail_row(i, c):
        take_row(edge + i, i)
        block_copy(i, i).start()
        wide.onto(edge + i)
        return c

    lax.fori_loop(0, HB, tail_row, 0)
    wide.send_spill(0)

    def head_row(b, c):
        slot = lax.rem(b, STAGES)
        take_row(b, slot)

        @pl.when(b + STAGES < edge)
        def _():
            block_copy(b + STAGES, slot).start()

        wide.onto(b)
        wide.across(b)
        return c

    lax.fori_loop(0, edge, head_row, 0)
    wide.halo_in(0)
    for b in range(edge, rows):
        wide.across(b)
    wide.take_in(0)

    zero = jnp.zeros((kvec, bs), F32)

    def first_sums(b, c):
        x = fw[b, 0:kvec]
        im = accw[b, 0:kvec]
        fim[b] = im
        fhw[b] = accw[b, kvec:2 * kvec]
        return c[0] + x * im, c[1] + x * x

    num, den = lax.fori_loop(0, rows, first_sums, (zero, zero))
    total_of = lambda x: jnp.sum(x, axis=1, keepdims=True)
    red_start(0, total_of(num), total_of(den))

    for k in range(ITERS):
        n = k + 1
        field = fim if k == 0 else fa

        def prepare(b, field=field):
            z = precondition(field[b], b)
            fz[b] = z
            thin.put(b, z)
            thin.diag(b, z)

        for b in range(HB):
            prepare(b)
        z_copy(n).start()
        thin.clear_tail()
        for b in range(edge, rows):
            prepare(b)
        for b in range(edge, rows):
            thin.onto(b)
        thin.send_spill(n)

        def interior(g, c, prepare=prepare):
            for t in range(4):
                prepare(4 + 4 * g + t)
            return c

        lax.fori_loop(0, (edge - HB) // 4, interior, 0)
        red_mid(k)

        def body(g, c):
            for t in range(4):
                thin.onto(4 * g + t)
            for t in range(4):
                thin.across(4 * g + t)
            return c

        lax.fori_loop(0, edge // 4, body, 0)
        thin.halo_in(n)
        for b in range(edge, rows):
            thin.across(b)
        thin.take_in(n)
        z_copy(n).wait_send()
        top, bottom = red_end(k)
        if k == 0:
            qb[...] = jnp.broadcast_to(top / bottom, (kvec, bs))
        else:
            sb[...] = jnp.broadcast_to(top / (bottom + 1.0), (kvec, bs))

        def update(b, c, k=k):
            z, hz = fz[b], acc[b]
            q = qb[...]
            if k == 0:
                u = q * fw[b, kvec:2 * kvec] - z
                hu = q * fhw[b] - hz
                r = q * fw[b, 0:kvec] - fim[b]
                a = hu - q * u
                fu[b] = u
                fhu[b] = hu
                fr[b] = r
            else:
                m = hz - q * z
                s = sb[...]
                u, hu, a = fu[b], fhu[b], fa[b]
                r = fr[b] - s * a
                fr[b] = r
                if k == 1:
                    fc[b] = s * u
                    fh[b] = s * hu
                else:
                    fc[b] = fc[b] + s * u
                    fh[b] = fh[b] + s * hu
                a = a - s * m
                fu[b] = u - s * z
                fhu[b] = hu - s * hz
            fa[b] = a
            return c[0] + a * r, c[1] + a * a

        cross, own = lax.fori_loop(0, rows, update, (zero, zero))
        if k + 1 < ITERS:
            red_start(k + 1, total_of(cross), total_of(own))

    def put_out(b, c):
        at = pl.ds(pl.multiple_of(b * bs, bs), bs)
        pltpu.make_async_copy(fc.at[b], c_out.at[:, at], out_sem.at[0]).start()
        pltpu.make_async_copy(fu.at[b], u_out.at[:, at], out_sem.at[1]).start()
        return c

    pltpu.make_async_copy(fpv, fpv, load_sem.at[1]).wait()
    pltpu.make_async_copy(fpi, fpi, load_sem.at[2]).wait()
    gram[...] = jnp.zeros_like(gram)

    def products(b, c):
        xh, xl = split(jnp.concatenate([fw[b, 0:kvec], fpv[b], fc[b], fu[b]], axis=0))
        yh, yl = split(jnp.concatenate([fim[b], fpi[b], fh[b], fhu[b]], axis=0))
        part = mmt(jnp.concatenate([xh, xl], axis=0), jnp.concatenate([xh, yh], axis=0))
        m = xh.shape[0]
        gram[...] = gram[...] + (part[0:m] + part[m:] + mmt(xh, jnp.concatenate([xl, yl], axis=0)))
        return c

    lax.fori_loop(0, rows, products, 0)
    span = lax.broadcasted_iota(jnp.int32, (kvec, 128), 1)
    for p in range(4):
        at = pl.ds(p * kvec, kvec)
        g = gram[at, 0:128]
        if p == 0:
            g = jnp.where(span == 96, total_of(cross), jnp.where(span == 97, total_of(own), g))
        parts[p] = g
        parts[4 + p] = gram[at, 128:256]

    def big1_copy(j):
        to = lax.rem(low + j, LOW)
        return rcopy(parts.at[to], big1.at[low], b1s.at[j], b1r.at[low], high * LOW + to)

    def big1_in(j):
        frm = lax.rem(low + j, LOW)
        return rcopy(parts.at[frm], big1.at[frm], b1s.at[j], b1r.at[frm], left)

    def big2_copy(j):
        to = lax.rem(high + j, n_high) * LOW + low
        return rcopy(big2.at[high], big2.at[high], b2s.at[j], b2r.at[high], to)

    def big2_in(j):
        frm = lax.rem(high + j, n_high)
        return rcopy(big2.at[frm], big2.at[frm], b2s.at[j], b2r.at[frm], left)

    def fin_copy(j):
        to = high * LOW + lax.rem(low + j, LOW)
        return rcopy(fin.at[low], fin.at[low], b3s.at[j], b3r.at[low], to)

    def fin_in(j):
        frm = lax.rem(low + j, LOW)
        return rcopy(fin.at[frm], fin.at[frm], b3s.at[j], b3r.at[frm], left)

    for j in range(1, LOW):
        big1_copy(j).start()
    lax.fori_loop(0, rows, put_out, 0)
    big1[low] = parts[low]
    for j in range(1, LOW):
        big1_in(j).wait_recv()
    tile = big1[0]
    for l in range(1, LOW):
        tile = tile + big1[l]
    big2[high] = tile
    for j in range(1, n_high):
        big2_copy(j).start()
    for j in range(1, n_high):
        big2_in(j).wait_recv()
    tile = big2[0]
    for l in range(1, n_high):
        tile = tile + big2[l]
    fin[low] = tile
    for j in range(1, LOW):
        fin_copy(j).start()
    for j in range(1, LOW):
        fin_in(j).wait_recv()

    for p in range(8):
        mats[p] = fin[p]
    pltpu.make_async_copy(fc, fc, out_sem.at[0]).wait()
    pltpu.make_async_copy(fu, fu, out_sem.at[1]).wait()

    for j in range(1, LOW):
        big1_copy(j).wait_send()
        fin_copy(j).wait_send()
    for j in range(1, n_high):
        big2_copy(j).wait_send()
    z_copy(0).wait_send()
    for n in range(ITERS + 1):
        spill_copy(n).wait_send()


def finish(kvec, c_in, u_in, fin, corr, reduced, cbuf, ubuf, aug, sem):
    first = pltpu.make_async_copy(c_in, cbuf, sem.at[0])
    second = pltpu.make_async_copy(u_in, ubuf, sem.at[1])
    first.start()
    second.start()
    head = fin[0]
    step = head[:, 96:97] / (head[:, 97:98] + 1.0)
    wide = jnp.broadcast_to(step, (kvec, 512))
    first.wait()
    second.wait()

    def add(g, c):
        at = pl.ds(pl.multiple_of(g * 512, 512), 512)
        cbuf[:, at] = cbuf[:, at] + wide * ubuf[:, at]
        return c

    lax.fori_loop(0, cbuf.shape[1] // 512, add, 0)
    third = pltpu.make_async_copy(cbuf, corr, sem.at[2])
    third.start()
    full = reduce_basis([fin[p] for p in range(4)], [fin[p] for p in range(4, 8)], step, aug, kvec)
    reduced[...] = full[:, 0:3 * kvec]
    third.wait()


def local(n_dev, blocks, block_cols, live_counts, onsite_energy, precond, vectors, prev_vectors, prev_image):
    rows, slots, bs = blocks.shape[0], blocks.shape[1], blocks.shape[2]
    kvec = vectors.shape[0]
    n_high = n_dev // LOW
    field = pltpu.VMEM((rows, kvec, bs), F32)
    tiles = pltpu.VMEM((rows * slots, bs, bs), BF16)
    dma = pltpu.SemaphoreType.DMA
    hbm = pl.BlockSpec(memory_space=pl.ANY)
    smem = pl.BlockSpec(memory_space=pltpu.SMEM)
    vmem = pl.BlockSpec(memory_space=pltpu.VMEM)

    def run(*args):
        return kernel(n_dev, rows, kvec, bs, *args)

    mid, last, mats = pl.pallas_call(
        run,
        out_shape=(
            jax.ShapeDtypeStruct(vectors.shape, F32),
            jax.ShapeDtypeStruct(vectors.shape, F32),
            jax.ShapeDtypeStruct((8, kvec, 128), F32),
        ),
        in_specs=[smem, smem, hbm, vmem, hbm, hbm, hbm, hbm],
        out_specs=(hbm, hbm, vmem),
        scratch_shapes=[
            pltpu.VMEM((STAGES, slots, bs, bs), F32),
            tiles, tiles, tiles, tiles,
            pltpu.VMEM((rows, bs, bs), BF16),
            pltpu.VMEM((rows, bs, bs), BF16),
            pltpu.SMEM((rows * slots,), jnp.int32),
            pltpu.VMEM((rows, 2 * kvec, bs), F32),
            field, field, field, field, field, field, field, field, field, field, field,
            pltpu.VMEM((rows + HB, 4 * kvec, bs), BF16),
            pltpu.VMEM((rows + HB, 2 * kvec, bs), F32),
            pltpu.VMEM((rows + HB, 2 * kvec, bs), BF16),
            pltpu.VMEM((rows + HB, kvec, bs), F32),
            pltpu.VMEM((kvec, bs), F32),
            pltpu.VMEM((kvec, bs), F32),
            pltpu.VMEM((ITERS, HB, kvec, bs), F32),
            pltpu.VMEM((ITERS, HB, kvec, bs), F32),
            pltpu.VMEM((ITERS, HB, kvec, bs), F32),
            pltpu.VMEM((HB, 2 * kvec, bs), F32),
            pltpu.VMEM((HB, 2 * kvec, bs), F32),
            pltpu.VMEM((HB, 2 * kvec, bs), F32),
            pltpu.VMEM((ITERS, LOW, 8, 128), F32),
            pltpu.VMEM((ITERS, n_high, 8, 128), F32),
            pltpu.VMEM((4 * kvec, 256), F32),
            pltpu.VMEM((8, kvec, 128), F32),
            pltpu.VMEM((LOW, kvec, 128), F32),
            pltpu.VMEM((n_high, kvec, 128), F32),
            pltpu.VMEM((8, kvec, 128), F32),
            dma((STAGES,)), dma((3,)), dma((2,)),
            dma((ITERS + 1,)), dma((ITERS + 1,)), dma((ITERS + 1,)), dma((ITERS + 1,)),
            dma((ITERS, LOW)), dma((ITERS, LOW)), dma((ITERS, n_high)), dma((ITERS, n_high)),
            dma((LOW,)), dma((LOW,)), dma((n_high,)), dma((n_high,)), dma((LOW,)), dma((LOW,)),
        ],
        compiler_params=pltpu.CompilerParams(
            collective_id=0, has_side_effects=True, vmem_limit_bytes=63 * 1024 * 1024
        ),
    )(block_cols.T, live_counts, blocks, onsite_energy.reshape(rows, 1, bs), precond, vectors, prev_vectors, prev_image)

    def run_last(*args):
        return finish(kvec, *args)

    return pl.pallas_call(
        run_last,
        out_shape=(
            jax.ShapeDtypeStruct(vectors.shape, F32),
            jax.ShapeDtypeStruct((3 * kvec, 3 * kvec), F32),
        ),
        in_specs=[hbm, hbm, vmem],
        out_specs=(hbm, vmem),
        scratch_shapes=[
            pltpu.VMEM(vectors.shape, F32),
            pltpu.VMEM(vectors.shape, F32),
            pltpu.VMEM((3 * kvec, 256), F32),
            dma((3,)),
        ],
    )(mid, last, mats)


def solution(mesh):
    n_dev = mesh.shape["rows"]

    def step(*args):
        return local(n_dev, *args)

    return jax.shard_map(
        step,
        mesh=mesh,
        in_specs=(
            P("rows", None, None, None), P("rows", None), P("rows"), P("rows"),
            P("rows", None, None), P(None, "rows"), P(None, "rows"), P(None, "rows"),
        ),
        out_specs=(P(None, "rows"), P()),
        check_vma=False,
    )
```

```python
import jax
import jax.numpy as jnp
from jax import lax
from jax.experimental import pallas as pl
from jax.experimental.pallas import tpu as pltpu
from jax.sharding import PartitionSpec as P

MESH = pl.DeviceIdType.MESH
F32 = jnp.float32
BF16 = jnp.bfloat16
HB = 4
ITERS = 3
LOW = 8
SLOTS = 4
STAGES = 4


def split(x):
    high = x.astype(BF16)
    return high, (x - high.astype(F32)).astype(BF16)


def mm(a, b):
    return jnp.dot(a, b, preferred_element_type=F32)


def mmt(a, b):
    return lax.dot_general(a, b, (((1,), (1,)), ((), ())), preferred_element_type=F32)


def reduce_basis(early, late, step, aug, kvec, between):
    width = 128
    size = 3 * kvec
    lane = lax.broadcasted_iota(jnp.int32, (kvec, width), 1)
    row = lax.broadcasted_iota(jnp.int32, (kvec, width), 0)
    step_col = jnp.sum(jnp.where(lane == row + 2 * kvec, step, 0.0), axis=0, keepdims=True)
    rest = jnp.zeros((2 * kvec, width), F32)

    def turned(x):
        return jnp.concatenate([rest, x, jnp.zeros((kvec, width), F32)], axis=0).T

    lead = lane < 2 * kvec
    side = (lane >= 2 * kvec) & (lane < size)
    g_c, g_u, p_c, p_u = late
    mixed = g_c + step * g_u
    flip = turned(jnp.where(lead, mixed, g_u))
    square = mixed + step_col * (flip[2 * kvec:size] + step * pltpu.roll(g_u, width - kvec, 1))
    tail = jnp.where(side, square, jnp.where(lead, mixed, 0.0))
    for g in range(2):
        a = jnp.where(lead, early[g], jnp.where(side, flip[g * kvec:(g + 1) * kvec], 0.0))
        aug[g * kvec:(g + 1) * kvec, 0:width] = a + jnp.where(lane == row + g * kvec, 1.0, 0.0)
    aug[2 * kvec:size, 0:width] = tail + jnp.where(lane == row + 2 * kvec, 1.0, 0.0)
    for g in range(3):
        aug[g * kvec:(g + 1) * kvec, width:2 * width] = jnp.where(lane == row + g * kvec, 1.0, 0.0)
    mixed = p_c + step * p_u
    cross = pltpu.roll(g_c + step * p_c, 2 * kvec, 1)
    flip = turned(jnp.where(lane < kvec, mixed, jnp.where(lead, cross, p_u)))
    square = mixed + step_col * (flip[2 * kvec:size] + step * pltpu.roll(p_u, width - kvec, 1))
    x = []
    for g in range(2):
        moved = pltpu.roll(early[g], 2 * kvec, 1)
        x.append(jnp.where(lead, moved, jnp.where(side, flip[g * kvec:(g + 1) * kvec], 0.0)))
    x.append(jnp.where(side, square, jnp.where(lead, mixed, 0.0)))
    x = jnp.concatenate(x + [jnp.zeros((kvec, width), F32)], axis=0)

    sub = lax.broadcasted_iota(jnp.int32, (8, width), 0)
    for top in range(0, size, 8):
        if top == 2 * kvec:
            between()
        n = size - top
        cols = [jnp.broadcast_to(aug[top:size, top + c:top + c + 1], (n, width)) for c in range(8)]
        pivot_rows = aug[top:top + 8, :]
        facs = []
        for j in range(8):
            f = cols[j] * (1.0 / cols[j][j:j + 1, :])
            head = jnp.where(sub > j, f[0:8], 0.0)
            facs.append(f)
            for c in range(j + 1, 8):
                pr = cols[c][j:j + 1, :]
                new_head = cols[c][0:8] - head * pr
                cols[c] = new_head if n == 8 else jnp.concatenate([new_head, cols[c][8:] - f[8:] * pr], axis=0)
            both = jnp.concatenate([head, head], axis=1)
            pivot_rows = pivot_rows - both * pivot_rows[j:j + 1, :]
        aug[top:top + 8, :] = pivot_rows
        for r in range(top + 8, size, 8):
            block = aug[r:r + 8, :]
            for j in range(8):
                f = facs[j][r - top:r - top + 8]
                block = block - jnp.concatenate([f, f], axis=1) * pivot_rows[j:j + 1, :]
            aug[r:r + 8, :] = block

    at = lax.broadcasted_iota(jnp.int32, (size, width), 1)
    diagonal = jnp.where(at == lax.broadcasted_iota(jnp.int32, (size, width), 0), aug[:, 0:width], 0.0)
    by_row = lax.rsqrt(jnp.sum(diagonal, axis=1, keepdims=True))
    by_col = jnp.sum(diagonal, axis=0, keepdims=True)
    by_col = jnp.where(at[0:1] < size, lax.rsqrt(jnp.where(at[0:1] < size, by_col, 1.0)), 0.0)
    w = aug[:, width:2 * width]
    w_full = jnp.concatenate([w, jnp.zeros((kvec, width), F32)], axis=0)
    half = jnp.dot(w, x, precision=lax.Precision.HIGHEST, preferred_element_type=F32)
    full = lax.dot_general(half, w_full, (((1,), (1,)), ((), ())), precision=lax.Precision.HIGHEST, preferred_element_type=F32)
    return full * by_row * by_col


def kernel(
    n_dev, rows, kvec, bs,
    cols, live, blocks, onsite, precond, vec, pvec, pimg,
    c_out, u_out, early_out, late_out, sums_out,
    stage, bh, bl, th, tl, ph, plo, offs,
    fw, fhw, fpv, fpi, fim, fr, fu, fhu, fa, fz, fc, fh, zsw, accw, zs, acc, qb, sb,
    zhalo, inc, spill, zhalo0, inc0, spill0, red1, red2, gram, early, early1, early2, early3, parts, big1, big2, fin,
    stage_sem, load_sem, out_sem, zs_sem, zr_sem, ss_sem, sr_sem,
    r1s, r1r, r2s, r2r, b1s, b1r, b2s, b2r, b3s, b3r, e1s, e1r, e2s, e2r, e3s, e3r,
):
    me = lax.axis_index("rows")
    low = lax.rem(me, LOW)
    high = lax.div(me, LOW)
    n_high = n_dev // LOW
    total = n_dev * rows
    first = me * rows
    right = lax.rem(me + 1, n_dev)
    left = lax.rem(me + n_dev - 1, n_dev)
    edge = rows - HB

    def field_copy(hbm, b):
        return hbm.at[:, pl.ds(b * bs, bs)]

    def block_copy(row, slot):
        return pltpu.make_async_copy(blocks.at[row], stage.at[slot], stage_sem.at[slot])

    def precond_copy(j):
        return pltpu.make_async_copy(precond.at[pl.ds(j * SLOTS, SLOTS)], stage.at[j], stage_sem.at[j])

    def start_loads(b, c):
        at = pl.ds(pl.multiple_of(b * bs, bs), bs)
        pltpu.make_async_copy(vec.at[:, at], fw.at[b, pl.ds(0, kvec)], load_sem.at[0]).start()
        return c

    lax.fori_loop(0, rows, start_loads, 0)
    for j in range(STAGES):
        precond_copy(j).start()

    def start_more(b, c):
        at = pl.ds(pl.multiple_of(b * bs, bs), bs)
        pltpu.make_async_copy(pvec.at[:, at], fpv.at[b], load_sem.at[1]).start()
        pltpu.make_async_copy(pimg.at[:, at], fpi.at[b], load_sem.at[2]).start()
        return c

    barrier = pltpu.get_barrier_semaphore()
    peers = [left, right]
    peers += [high * LOW + lax.rem(low + j, LOW) for j in range(1, LOW)]
    peers += [lax.rem(high + j, n_high) * LOW + low for j in range(1, n_high)]
    for peer in peers:
        pl.semaphore_signal(barrier, inc=1, device_id=(peer,), device_id_type=MESH)

    def rcopy(src, dst, s_sem, r_sem, to):
        return pltpu.make_async_remote_copy(
            src_ref=src, dst_ref=dst, send_sem=s_sem, recv_sem=r_sem,
            device_id=(to,), device_id_type=MESH,
        )

    def z_copy(n):
        src, dst = (fw, zhalo0) if n == 0 else (fz, zhalo.at[n - 1])
        return rcopy(src.at[pl.ds(0, HB)], dst, zs_sem.at[n], zr_sem.at[n], left)

    def spill_copy(n):
        src, dst = (spill0, inc0) if n == 0 else (spill.at[n - 1], inc.at[n - 1])
        return rcopy(src, dst, ss_sem.at[n], sr_sem.at[n], right)

    def low_copy(i, j):
        to = high * LOW + lax.rem(low + j, LOW)
        return rcopy(red1.at[i, low], red1.at[i, low], r1s.at[i, j], r1r.at[i, low], to)

    def low_in(i, j):
        frm = lax.rem(low + j, LOW)
        return rcopy(red1.at[i, frm], red1.at[i, frm], r1s.at[i, j], r1r.at[i, frm], left)

    def high_copy(i, j):
        to = lax.rem(high + j, n_high) * LOW + low
        return rcopy(red2.at[i, high], red2.at[i, high], r2s.at[i, j], r2r.at[i, high], to)

    def high_in(i, j):
        frm = lax.rem(high + j, n_high)
        return rcopy(red2.at[i, frm], red2.at[i, frm], r2s.at[i, j], r2r.at[i, frm], left)

    lane = lax.broadcasted_iota(jnp.int32, (8, 128), 1)
    groups = kvec // 8

    def pack(a, b):
        tile = jnp.zeros((8, 128), F32)
        for g in range(groups):
            tile = tile + jnp.where(lane == g, a[8 * g:8 * g + 8], 0.0)
            tile = tile + jnp.where(lane == groups + g, b[8 * g:8 * g + 8], 0.0)
        return tile

    def unpack(tile):
        out = []
        for base in (0, groups):
            out.append(jnp.concatenate(
                [jnp.sum(jnp.where(lane == base + g, tile, 0.0), axis=1, keepdims=True) for g in range(groups)],
                axis=0,
            ))
        return out

    def red_start(i, a, b):
        red1[i, low] = pack(a, b)
        for j in range(1, LOW):
            low_copy(i, j).start()

    def red_mid(i):
        for j in range(1, LOW):
            low_in(i, j).wait_recv()
        tile = red1[i, 0]
        for l in range(1, LOW):
            tile = tile + red1[i, l]
        red2[i, high] = tile
        for j in range(1, n_high):
            high_copy(i, j).start()

    def red_end(i):
        for j in range(1, n_high):
            high_in(i, j).wait_recv()
        tile = red2[i, 0]
        for l in range(1, n_high):
            tile = tile + red2[i, l]
        for j in range(1, LOW):
            low_copy(i, j).wait_send()
        for j in range(1, n_high):
            high_copy(i, j).wait_send()
        return unpack(tile)

    class Exchange:
        def __init__(self, src, near, far, out, sems):
            self.src, self.near, self.far, self.out, self.sems = src, near, far, out, sems

        def near_copy(self, j):
            to = lax.rem(low + j, LOW)
            return rcopy(self.src.at[to], self.near.at[low], self.sems[0].at[j], self.sems[1].at[low], high * LOW + to)

        def near_in(self, j):
            frm = lax.rem(low + j, LOW)
            return rcopy(self.src.at[frm], self.near.at[frm], self.sems[0].at[j], self.sems[1].at[frm], left)

        def far_copy(self, j):
            to = lax.rem(high + j, n_high) * LOW + low
            return rcopy(self.far.at[high], self.far.at[high], self.sems[2].at[j], self.sems[3].at[high], to)

        def far_in(self, j):
            frm = lax.rem(high + j, n_high)
            return rcopy(self.far.at[frm], self.far.at[frm], self.sems[2].at[j], self.sems[3].at[frm], left)

        def back_copy(self, j):
            to = high * LOW + lax.rem(low + j, LOW)
            return rcopy(self.out.at[low], self.out.at[low], self.sems[4].at[j], self.sems[5].at[low], to)

        def back_in(self, j):
            frm = lax.rem(low + j, LOW)
            return rcopy(self.out.at[frm], self.out.at[frm], self.sems[4].at[j], self.sems[5].at[frm], left)

        def start(self):
            for j in range(1, LOW):
                self.near_copy(j).start()
            self.near[low] = self.src[low]

        def middle(self):
            for j in range(1, LOW):
                self.near_in(j).wait_recv()
            tile = self.near[0]
            for l in range(1, LOW):
                tile = tile + self.near[l]
            self.far[high] = tile
            for j in range(1, n_high):
                self.far_copy(j).start()

        def back(self):
            for j in range(1, n_high):
                self.far_in(j).wait_recv()
            tile = self.far[0]
            for l in range(1, n_high):
                tile = tile + self.far[l]
            self.out[low] = tile
            for j in range(1, LOW):
                self.back_copy(j).start()

        def end(self):
            for j in range(1, LOW):
                self.back_in(j).wait_recv()

        def drain(self):
            for j in range(1, LOW):
                self.near_copy(j).wait_send()
                self.back_copy(j).wait_send()
            for j in range(1, n_high):
                self.far_copy(j).wait_send()

    soon = Exchange(early, early1, early2, early3, (e1s, e1r, e2s, e2r, e3s, e3r))
    later = Exchange(parts, big1, big2, fin, (b1s, b1r, b2s, b2r, b3s, b3r))

    class Apply:
        def __init__(self, kv, parts_ref, acc_ref):
            self.kv, self.zs, self.acc = kv, parts_ref, acc_ref

        def put(self, b, z):
            zh, zl = split(z)
            self.zs[b, 0:self.kv, :] = zh
            self.zs[b, self.kv:2 * self.kv, :] = zl

        def diag(self, b, z):
            self.acc[b] = onsite[b] * z

        def clear_tail(self):
            for t in range(HB):
                self.acc[rows + t] = jnp.zeros((self.kv, bs), F32)

        def product(self, z, hi, lo):
            part = mm(z, hi)
            return part[0:self.kv] + part[self.kv:] + mm(z[0:self.kv], lo)

        def onto(self, b):
            zb = self.zs[b]
            sums = [None] * (HB + 1)
            for s in range(SLOTS):
                moved = self.product(zb, bh[b * SLOTS + s], bl[b * SLOTS + s])
                off = offs[b * SLOTS + s]
                for o in range(HB + 1):
                    term = jnp.where(off == o, 1.0, 0.0) * moved
                    sums[o] = term if sums[o] is None else sums[o] + term
            for o in range(HB + 1):
                self.acc[b + o] = self.acc[b + o] + sums[o]

        def across(self, b):
            out = None
            for s in range(SLOTS):
                term = self.product(self.zs[b + offs[b * SLOTS + s]], th[b * SLOTS + s], tl[b * SLOTS + s])
                out = term if out is None else out + term
            self.acc[b] = self.acc[b] + out

        def halo_in(self, n):
            z_copy(n).wait_recv()
            for t in range(HB):
                self.put(rows + t, zhalo0[t] if n == 0 else zhalo[n - 1, t])

        def send_spill(self, n):
            for t in range(HB):
                if n == 0:
                    spill0[t] = self.acc[rows + t]
                else:
                    spill[n - 1, t] = self.acc[rows + t]
            spill_copy(n).start()

        def take_in(self, n):
            spill_copy(n).wait_recv()
            for t in range(HB):
                self.acc[t] = self.acc[t] + (inc0[t] if n == 0 else inc[n - 1, t])

    wide = Apply(2 * kvec, zsw, accw)
    thin = Apply(kvec, zs, acc)

    def precondition(x, b):
        dh, dl = split(x)
        part = mm(jnp.concatenate([dh, dl], axis=0), ph[b])
        return part[0:kvec] + part[kvec:] + mm(dh, plo[b])

    pltpu.make_async_copy(fw.at[:, pl.ds(0, kvec)], fw.at[:, pl.ds(0, kvec)], load_sem.at[0]).wait()
    for j in range(rows // SLOTS):
        precond_copy(j).wait()
        for t in range(SLOTS):
            b = j * SLOTS + t
            xh, xl = split(stage[j, t])
            ph[b] = xh.T
            plo[b] = xl.T
        block_copy(edge + j, j).start()
        for t in range(SLOTS):
            b = j * SLOTS + t
            v = fw[b, 0:kvec]
            fw[b, kvec:2 * kvec] = precondition(v, b)
            x = fw[b]
            wide.put(b, x)
            wide.diag(b, x)
        if j == 0:
            pl.semaphore_wait(barrier, len(peers))
            z_copy(0).start()
    lax.fori_loop(0, rows, start_more, 0)
    wide.clear_tail()

    def take_row(b, slot):
        block_copy(b, slot).wait()
        for s in range(SLOTS):
            off = cols[s, b] - first - b
            off = jnp.where(off < 0, off + total, off)
            offs[b * SLOTS + s] = jnp.minimum(off, HB)
            alive = jnp.where(s < live[b], 1.0, 0.0)
            xh, xl = split(stage[slot, s] * alive)
            bh[b * SLOTS + s] = xh
            bl[b * SLOTS + s] = xl
            th[b * SLOTS + s] = xh.T
            tl[b * SLOTS + s] = xl.T

    def tail_row(i, c):
        take_row(edge + i, i)
        block_copy(i, i).start()
        wide.onto(edge + i)
        return c

    lax.fori_loop(0, HB, tail_row, 0)
    wide.send_spill(0)

    def head_row(b, c):
        slot = lax.rem(b, STAGES)
        take_row(b, slot)

        @pl.when(b + STAGES < edge)
        def _():
            block_copy(b + STAGES, slot).start()

        wide.onto(b)
        wide.across(b)
        return c

    lax.fori_loop(0, edge, head_row, 0)
    wide.halo_in(0)
    for b in range(edge, rows):
        wide.across(b)
    wide.take_in(0)

    zero = jnp.zeros((kvec, bs), F32)

    def first_sums(b, c):
        x = fw[b, 0:kvec]
        im = accw[b, 0:kvec]
        fim[b] = im
        fhw[b] = accw[b, kvec:2 * kvec]
        return c[0] + x * im, c[1] + x * x

    num, den = lax.fori_loop(0, rows, first_sums, (zero, zero))
    total_of = lambda x: jnp.sum(x, axis=1, keepdims=True)
    red_start(0, total_of(num), total_of(den))

    pltpu.make_async_copy(fpv, fpv, load_sem.at[1]).wait()
    pltpu.make_async_copy(fpi, fpi, load_sem.at[2]).wait()

    def old_products(b, c):
        xh, xl = split(jnp.concatenate([fw[b, 0:kvec], fpv[b], fim[b], fpi[b]], axis=0))
        m = 2 * kvec
        part = mmt(jnp.concatenate([xh[0:m], xl[0:m]], axis=0), xh)
        return c + (part[0:m] + part[m:] + mmt(xh[0:m], xl))

    old = lax.fori_loop(0, rows, old_products, jnp.zeros((2 * kvec, 128), F32))
    for p in range(8):
        early[p] = old[8 * p:8 * p + 8]
    soon.start()

    for k in range(ITERS):
        n = k + 1
        field = fim if k == 0 else fa

        def prepare(b, field=field):
            z = precondition(field[b], b)
            fz[b] = z
            thin.put(b, z)
            thin.diag(b, z)

        for b in range(HB):
            prepare(b)
        z_copy(n).start()
        thin.clear_tail()
        for b in range(edge, rows):
            prepare(b)
        for b in range(edge, rows):
            thin.onto(b)
        thin.send_spill(n)

        def interior(g, c, prepare=prepare):
            for t in range(4):
                prepare(4 + 4 * g + t)
            return c

        for g in range((edge - HB) // 4):
            interior(g, 0)
        red_mid(k)
        (soon.middle, soon.back, soon.end)[k]()

        def body(g, c):
            for t in range(4):
                thin.onto(4 * g + t)
            for t in range(4):
                thin.across(4 * g + t)
            return c

        for g in range(edge // 4):
            body(g, 0)
        thin.halo_in(n)
        for b in range(edge, rows):
            thin.across(b)
        thin.take_in(n)
        z_copy(n).wait_send()
        top, bottom = red_end(k)
        if k == 0:
            qb[...] = jnp.broadcast_to(top / bottom, (kvec, bs))
        else:
            sb[...] = jnp.broadcast_to(top / (bottom + 1.0), (kvec, bs))

        def update(b, c, k=k):
            z, hz = fz[b], acc[b]
            q = qb[...]
            if k == 0:
                u = q * fw[b, kvec:2 * kvec] - z
                hu = q * fhw[b] - hz
                r = q * fw[b, 0:kvec] - fim[b]
                a = hu - q * u
                fu[b] = u
                fhu[b] = hu
                fr[b] = r
            else:
                m = hz - q * z
                s = sb[...]
                u, hu, a = fu[b], fhu[b], fa[b]
                r = fr[b] - s * a
                fr[b] = r
                if k == 1:
                    fc[b] = s * u
                    fh[b] = s * hu
                else:
                    fc[b] = fc[b] + s * u
                    fh[b] = fh[b] + s * hu
                a = a - s * m
                fu[b] = u - s * z
                fhu[b] = hu - s * hz
            fa[b] = a
            return c[0] + a * r, c[1] + a * a

        cross, own = lax.fori_loop(0, rows, update, (zero, zero))
        if k + 1 < ITERS:
            red_start(k + 1, total_of(cross), total_of(own))

    def put_out(b, c):
        at = pl.ds(pl.multiple_of(b * bs, bs), bs)
        pltpu.make_async_copy(fc.at[b], c_out.at[:, at], out_sem.at[0]).start()
        pltpu.make_async_copy(fu.at[b], u_out.at[:, at], out_sem.at[1]).start()
        return c

    red_start(ITERS, total_of(cross), total_of(own))
    lax.fori_loop(0, rows, put_out, 0)

    gram[...] = jnp.zeros_like(gram)

    def products(b, c):
        xh, xl = split(jnp.concatenate([fw[b, 0:kvec], fpv[b], fc[b], fu[b]], axis=0))
        yh, yl = split(jnp.concatenate([fim[b], fpi[b], fh[b], fhu[b]], axis=0))
        m = 2 * kvec
        left_side = jnp.concatenate([xh[m:], yh[m:], xl[m:], yl[m:]], axis=0)
        part = mmt(left_side, jnp.concatenate([xh, yh], axis=0))
        n = 2 * m
        gram[...] = gram[...] + (part[0:n] + part[n:] + mmt(left_side[0:n], jnp.concatenate([xl, yl], axis=0)))
        return c

    lax.fori_loop(0, rows, products, 0)
    red_mid(ITERS)
    span = lax.broadcasted_iota(jnp.int32, (kvec, 128), 1)
    hp = pltpu.roll(gram[2 * kvec:3 * kvec, 0:128], 64, 1)
    hup = pltpu.roll(gram[3 * kvec:4 * kvec, 0:128], 64, 1)
    last = span >= 3 * kvec
    quarters = (
        jnp.where(last, hp, gram[0:kvec, 0:128]),
        gram[kvec:2 * kvec, 0:128],
        jnp.where(last, hup, gram[0:kvec, 128:256]),
        gram[kvec:2 * kvec, 128:256],
    )
    for p in range(4):
        parts[2 * p] = quarters[p][0:kvec // 2]
        parts[2 * p + 1] = quarters[p][kvec // 2:]
    later.start()
    later.middle()
    top, bottom = red_end(ITERS)
    sums_out[...] = jnp.broadcast_to(top / (bottom + 1.0), (kvec, 128))
    later.back()
    for p in range(8):
        early_out[p] = early3[p]
    later.end()
    for p in range(8):
        late_out[p] = fin[p]
    pltpu.make_async_copy(fc, fc, out_sem.at[0]).wait()
    pltpu.make_async_copy(fu, fu, out_sem.at[1]).wait()

    soon.drain()
    later.drain()
    z_copy(0).wait_send()
    for n in range(ITERS + 1):
        spill_copy(n).wait_send()


def finish(kvec, c_in, u_in, early, late, step_in, corr, reduced, cbuf, ubuf, aug, sem):
    first = pltpu.make_async_copy(c_in, cbuf, sem.at[0])
    second = pltpu.make_async_copy(u_in, ubuf, sem.at[1])
    third = pltpu.make_async_copy(cbuf, corr, sem.at[2])
    first.start()
    second.start()
    step = step_in[:, 0:1]

    def add_last():
        wide = jnp.broadcast_to(step, (kvec, 512))
        first.wait()
        second.wait()

        def add(g, c):
            at = pl.ds(pl.multiple_of(g * 512, 512), 512)
            cbuf[:, at] = cbuf[:, at] + wide * ubuf[:, at]
            return c

        lax.fori_loop(0, cbuf.shape[1] // 512, add, 0)
        third.start()

    quarter = lambda p: jnp.concatenate([late[2 * p], late[2 * p + 1]], axis=0)
    half = lambda g: jnp.concatenate([early[4 * g + p] for p in range(4)], axis=0)
    full = reduce_basis([half(0), half(1)], [quarter(p) for p in range(4)], step, aug, kvec, add_last)
    reduced[...] = full[:, 0:3 * kvec]
    third.wait()


def local(n_dev, blocks, block_cols, live_counts, onsite_energy, precond, vectors, prev_vectors, prev_image):
    rows, slots, bs = blocks.shape[0], blocks.shape[1], blocks.shape[2]
    kvec = vectors.shape[0]
    n_high = n_dev // LOW
    field = pltpu.VMEM((rows, kvec, bs), F32)
    tiles = pltpu.VMEM((rows * slots, bs, bs), BF16)
    dma = pltpu.SemaphoreType.DMA
    hbm = pl.BlockSpec(memory_space=pl.ANY)
    smem = pl.BlockSpec(memory_space=pltpu.SMEM)
    vmem = pl.BlockSpec(memory_space=pltpu.VMEM)

    def run(*args):
        return kernel(n_dev, rows, kvec, bs, *args)

    outs = pl.pallas_call(
        run,
        out_shape=(
            jax.ShapeDtypeStruct(vectors.shape, F32),
            jax.ShapeDtypeStruct(vectors.shape, F32),
            jax.ShapeDtypeStruct((8, 8, 128), F32),
            jax.ShapeDtypeStruct((8, kvec // 2, 128), F32),
            jax.ShapeDtypeStruct((kvec, 128), F32),
        ),
        in_specs=[smem, smem, hbm, vmem, hbm, hbm, hbm, hbm],
        out_specs=(hbm, hbm, vmem, vmem, vmem),
        scratch_shapes=[
            pltpu.VMEM((STAGES, slots, bs, bs), F32),
            tiles, tiles, tiles, tiles,
            pltpu.VMEM((rows, bs, bs), BF16),
            pltpu.VMEM((rows, bs, bs), BF16),
            pltpu.SMEM((rows * slots,), jnp.int32),
            pltpu.VMEM((rows, 2 * kvec, bs), F32),
            field, field, field, field, field, field, field, field, field, field, field,
            pltpu.VMEM((rows + HB, 4 * kvec, bs), BF16),
            pltpu.VMEM((rows + HB, 2 * kvec, bs), F32),
            pltpu.VMEM((rows + HB, 2 * kvec, bs), BF16),
            pltpu.VMEM((rows + HB, kvec, bs), F32),
            pltpu.VMEM((kvec, bs), F32),
            pltpu.VMEM((kvec, bs), F32),
            pltpu.VMEM((ITERS, HB, kvec, bs), F32),
            pltpu.VMEM((ITERS, HB, kvec, bs), F32),
            pltpu.VMEM((ITERS, HB, kvec, bs), F32),
            pltpu.VMEM((HB, 2 * kvec, bs), F32),
            pltpu.VMEM((HB, 2 * kvec, bs), F32),
            pltpu.VMEM((HB, 2 * kvec, bs), F32),
            pltpu.VMEM((ITERS + 1, LOW, 8, 128), F32),
            pltpu.VMEM((ITERS + 1, n_high, 8, 128), F32),
            pltpu.VMEM((4 * kvec, 256), F32),
            pltpu.VMEM((LOW, 8, 128), F32),
            pltpu.VMEM((LOW, 8, 128), F32),
            pltpu.VMEM((n_high, 8, 128), F32),
            pltpu.VMEM((LOW, 8, 128), F32),
            pltpu.VMEM((LOW, kvec // 2, 128), F32),
            pltpu.VMEM((LOW, kvec // 2, 128), F32),
            pltpu.VMEM((n_high, kvec // 2, 128), F32),
            pltpu.VMEM((LOW, kvec // 2, 128), F32),
            dma((STAGES,)), dma((3,)), dma((2,)),
            dma((ITERS + 1,)), dma((ITERS + 1,)), dma((ITERS + 1,)), dma((ITERS + 1,)),
            dma((ITERS + 1, LOW)), dma((ITERS + 1, LOW)), dma((ITERS + 1, n_high)), dma((ITERS + 1, n_high)),
            dma((LOW,)), dma((LOW,)), dma((n_high,)), dma((n_high,)), dma((LOW,)), dma((LOW,)),
            dma((LOW,)), dma((LOW,)), dma((n_high,)), dma((n_high,)), dma((LOW,)), dma((LOW,)),
        ],
        compiler_params=pltpu.CompilerParams(
            collective_id=0, has_side_effects=True, vmem_limit_bytes=63 * 1024 * 1024
        ),
    )(block_cols.T, live_counts, blocks, onsite_energy.reshape(rows, 1, bs), precond, vectors, prev_vectors, prev_image)

    def run_last(*args):
        return finish(kvec, *args)

    return pl.pallas_call(
        run_last,
        out_shape=(
            jax.ShapeDtypeStruct(vectors.shape, F32),
            jax.ShapeDtypeStruct((3 * kvec, 3 * kvec), F32),
        ),
        in_specs=[hbm, hbm, vmem, vmem, vmem],
        out_specs=(hbm, vmem),
        scratch_shapes=[
            pltpu.VMEM(vectors.shape, F32),
            pltpu.VMEM(vectors.shape, F32),
            pltpu.VMEM((3 * kvec, 256), F32),
            dma((3,)),
        ],
    )(*outs)


def solution(mesh):
    n_dev = mesh.shape["rows"]

    def step(*args):
        return local(n_dev, *args)

    return jax.shard_map(
        step,
        mesh=mesh,
        in_specs=(
            P("rows", None, None, None), P("rows", None), P("rows"), P("rows"),
            P("rows", None, None), P(None, "rows"), P(None, "rows"), P(None, "rows"),
        ),
        out_specs=(P(None, "rows"), P()),
        check_vma=False,
    )
```

```python
import jax
import jax.numpy as jnp
from jax import lax
from jax.experimental import pallas as pl
from jax.experimental.pallas import tpu as pltpu
from jax.sharding import PartitionSpec as P

MESH = pl.DeviceIdType.MESH
F32 = jnp.float32
BF16 = jnp.bfloat16
HB = 4
ITERS = 3
LOW = 8
SLOTS = 4
STAGES = 4


def split(x):
    high = x.astype(BF16)
    return high, (x - high.astype(F32)).astype(BF16)


def mm(a, b):
    return jnp.dot(a, b, preferred_element_type=F32)


def mmt(a, b):
    return lax.dot_general(a, b, (((1,), (1,)), ((), ())), preferred_element_type=F32)


def reduce_basis(early, late, step, aug, kvec, between):
    width = 128
    size = 3 * kvec
    lane = lax.broadcasted_iota(jnp.int32, (kvec, width), 1)
    row = lax.broadcasted_iota(jnp.int32, (kvec, width), 0)
    step_col = jnp.sum(jnp.where(lane == row + 2 * kvec, step, 0.0), axis=0, keepdims=True)
    rest = jnp.zeros((2 * kvec, width), F32)

    def turned(x):
        return jnp.concatenate([rest, x, jnp.zeros((kvec, width), F32)], axis=0).T

    lead = lane < 2 * kvec
    side = (lane >= 2 * kvec) & (lane < size)
    g_c, g_u, p_c, p_u = late
    mixed = g_c + step * g_u
    flip = turned(jnp.where(lead, mixed, g_u))
    square = mixed + step_col * (flip[2 * kvec:size] + step * pltpu.roll(g_u, width - kvec, 1))
    tail = jnp.where(side, square, jnp.where(lead, mixed, 0.0))
    for g in range(2):
        a = jnp.where(lead, early[g], jnp.where(side, flip[g * kvec:(g + 1) * kvec], 0.0))
        aug[g * kvec:(g + 1) * kvec, 0:width] = a + jnp.where(lane == row + g * kvec, 1.0, 0.0)
    aug[2 * kvec:size, 0:width] = tail + jnp.where(lane == row + 2 * kvec, 1.0, 0.0)
    for g in range(3):
        aug[g * kvec:(g + 1) * kvec, width:2 * width] = jnp.where(lane == row + g * kvec, 1.0, 0.0)
    mixed = p_c + step * p_u
    cross = pltpu.roll(g_c + step * p_c, 2 * kvec, 1)
    flip = turned(jnp.where(lane < kvec, mixed, jnp.where(lead, cross, p_u)))
    square = mixed + step_col * (flip[2 * kvec:size] + step * pltpu.roll(p_u, width - kvec, 1))
    x = []
    for g in range(2):
        moved = pltpu.roll(early[g], 2 * kvec, 1)
        x.append(jnp.where(lead, moved, jnp.where(side, flip[g * kvec:(g + 1) * kvec], 0.0)))
    x.append(jnp.where(side, square, jnp.where(lead, mixed, 0.0)))
    x = jnp.concatenate(x + [jnp.zeros((kvec, width), F32)], axis=0)

    sub = lax.broadcasted_iota(jnp.int32, (8, width), 0)
    for top in range(0, size, 8):
        if top == 2 * kvec:
            between()
        n = size - top
        cols = [jnp.broadcast_to(aug[top:size, top + c:top + c + 1], (n, width)) for c in range(8)]
        pivot_rows = aug[top:top + 8, :]
        facs = []
        for j in range(8):
            f = cols[j] * (1.0 / cols[j][j:j + 1, :])
            head = jnp.where(sub > j, f[0:8], 0.0)
            facs.append(f)
            for c in range(j + 1, 8):
                pr = cols[c][j:j + 1, :]
                new_head = cols[c][0:8] - head * pr
                cols[c] = new_head if n == 8 else jnp.concatenate([new_head, cols[c][8:] - f[8:] * pr], axis=0)
            both = jnp.concatenate([head, head], axis=1)
            pivot_rows = pivot_rows - both * pivot_rows[j:j + 1, :]
        aug[top:top + 8, :] = pivot_rows
        for r in range(top + 8, size, 8):
            block = aug[r:r + 8, :]
            for j in range(8):
                f = facs[j][r - top:r - top + 8]
                block = block - jnp.concatenate([f, f], axis=1) * pivot_rows[j:j + 1, :]
            aug[r:r + 8, :] = block

    at = lax.broadcasted_iota(jnp.int32, (size, width), 1)
    diagonal = jnp.where(at == lax.broadcasted_iota(jnp.int32, (size, width), 0), aug[:, 0:width], 0.0)
    by_row = lax.rsqrt(jnp.sum(diagonal, axis=1, keepdims=True))
    by_col = jnp.sum(diagonal, axis=0, keepdims=True)
    by_col = jnp.where(at[0:1] < size, lax.rsqrt(jnp.where(at[0:1] < size, by_col, 1.0)), 0.0)
    w = aug[:, width:2 * width]
    w_full = jnp.concatenate([w, jnp.zeros((kvec, width), F32)], axis=0)
    half = jnp.dot(w, x, precision=lax.Precision.HIGHEST, preferred_element_type=F32)
    full = lax.dot_general(half, w_full, (((1,), (1,)), ((), ())), precision=lax.Precision.HIGHEST, preferred_element_type=F32)
    return full * by_row * by_col


def kernel(
    n_dev, rows, kvec, bs,
    cols_in, live_in, blocks, onsite_in, precond, vec, pvec, pimg,
    c_out, u_out, early_out, late_out, sums_out,
    cols, live, onsite, stage, bh, bl, th, tl, ph, plo, offs,
    fw, fhw, fpv, fpi, fim, fr, fu, fhu, fa, fz, fc, fh, zsw, accw, zs, acc, qb, sb,
    zhalo, inc, spill, zhalo0, inc0, spill0, red1, red2, gram, early, early1, early2, early3, parts, big1, big2, fin,
    stage_sem, load_sem, out_sem, zs_sem, zr_sem, ss_sem, sr_sem,
    r1s, r1r, r2s, r2r, b1s, b1r, b2s, b2r, b3s, b3r, e1s, e1r, e2s, e2r, e3s, e3r,
):
    me = lax.axis_index("rows")
    low = lax.rem(me, LOW)
    high = lax.div(me, LOW)
    n_high = n_dev // LOW
    total = n_dev * rows
    first = me * rows
    right = lax.rem(me + 1, n_dev)
    left = lax.rem(me + n_dev - 1, n_dev)
    edge = rows - HB

    def field_copy(hbm, b):
        return hbm.at[:, pl.ds(b * bs, bs)]

    def block_copy(row, slot):
        return pltpu.make_async_copy(blocks.at[row], stage.at[slot], stage_sem.at[slot])

    def precond_copy(j):
        return pltpu.make_async_copy(precond.at[pl.ds(j * SLOTS, SLOTS)], stage.at[j], stage_sem.at[j])

    def start_loads(b, c):
        at = pl.ds(pl.multiple_of(b * bs, bs), bs)
        pltpu.make_async_copy(vec.at[:, at], fw.at[b, pl.ds(0, kvec)], load_sem.at[0]).start()
        return c

    smalls = [
        pltpu.make_async_copy(x, y, load_sem.at[3 + t])
        for t, (x, y) in enumerate(((cols_in, cols), (live_in, live), (onsite_in, onsite)))
    ]
    lax.fori_loop(0, rows, start_loads, 0)
    for j in range(STAGES):
        precond_copy(j).start()
    for copy in smalls:
        copy.start()

    barrier = pltpu.get_barrier_semaphore()
    others = n_dev // 2

    def greet(j, c):
        pl.semaphore_signal(barrier, inc=1, device_id=(lax.rem(me + 2 * j, n_dev),), device_id_type=MESH)
        return c

    lax.fori_loop(1, others, greet, 0)
    partner = me + 1 - 2 * lax.rem(me, 2)
    near_odd = [high * LOW + lax.rem(low + j, LOW) for j in range(1, LOW, 2)]
    for peer in [left, right] + near_odd:
        pl.semaphore_signal(barrier, inc=1, device_id=(peer,), device_id_type=MESH)
    n_greet = others - 1 + 2 + len(near_odd)

    def start_more(b, c):
        at = pl.ds(pl.multiple_of(b * bs, bs), bs)
        pltpu.make_async_copy(pvec.at[:, at], fpv.at[b], load_sem.at[1]).start()
        pltpu.make_async_copy(pimg.at[:, at], fpi.at[b], load_sem.at[2]).start()
        return c

    def rcopy(src, dst, s_sem, r_sem, to):
        return pltpu.make_async_remote_copy(
            src_ref=src, dst_ref=dst, send_sem=s_sem, recv_sem=r_sem,
            device_id=(to,), device_id_type=MESH,
        )

    def z_copy(n):
        src, dst = (fw, zhalo0) if n == 0 else (fz, zhalo.at[n - 1])
        return rcopy(src.at[pl.ds(0, HB)], dst, zs_sem.at[n], zr_sem.at[n], left)

    def spill_copy(n):
        src, dst = (spill0, inc0) if n == 0 else (spill.at[n - 1], inc.at[n - 1])
        return rcopy(src, dst, ss_sem.at[n], sr_sem.at[n], right)

    def pair_copy(i):
        return rcopy(red1.at[i, 0], red1.at[i, 1], r1s.at[i], r1r.at[i], partner)

    def chip_copy(i, j):
        at = red2.at[i, lax.div(me, 2)]
        return rcopy(at, at, r2s.at[i], r2r.at[i], lax.rem(me + 2 * j, n_dev))

    span = lax.broadcasted_iota(jnp.int32, (kvec, 128), 1)
    rank = lax.broadcasted_iota(jnp.int32, (kvec, 128), 0)

    def red_start(i, a, b):
        both = jnp.where(span == rank, a, 0.0) + jnp.where(span == rank + kvec, b, 0.0)
        red1[i, 0] = jnp.sum(both, axis=0, keepdims=True)
        pair_copy(i).start()

    def red_mid(i):
        pair_copy(i).wait_recv()
        red2[i, lax.div(me, 2)] = red1[i, 0] + red1[i, 1]

        def send(j, c):
            chip_copy(i, j).start()
            return c

        lax.fori_loop(1, others, send, 0)

    def red_end(i):
        got = red2.at[i, pl.ds(0, others - 1)]
        pltpu.make_async_copy(got, got, r2r.at[i]).wait()
        pltpu.make_async_copy(got, got, r2s.at[i]).wait()
        pair_copy(i).wait_send()
        line = jnp.broadcast_to(jnp.sum(red2[i], axis=0), (kvec, 128))
        top = jnp.sum(jnp.where(span == rank, line, 0.0), axis=1, keepdims=True)
        bottom = jnp.sum(jnp.where(span == rank + kvec, line, 0.0), axis=1, keepdims=True)
        return top, bottom

    class Exchange:
        def __init__(self, src, near, far, out, sems):
            self.src, self.near, self.far, self.out, self.sems = src, near, far, out, sems

        def near_copy(self, j):
            to = lax.rem(low + j, LOW)
            return rcopy(self.src.at[to], self.near.at[low], self.sems[0].at[j], self.sems[1].at[low], high * LOW + to)

        def near_in(self, j):
            frm = lax.rem(low + j, LOW)
            return rcopy(self.src.at[frm], self.near.at[frm], self.sems[0].at[j], self.sems[1].at[frm], left)

        def far_copy(self, j):
            to = lax.rem(high + j, n_high) * LOW + low
            return rcopy(self.far.at[high], self.far.at[high], self.sems[2].at[j], self.sems[3].at[high], to)

        def far_in(self, j):
            frm = lax.rem(high + j, n_high)
            return rcopy(self.far.at[frm], self.far.at[frm], self.sems[2].at[j], self.sems[3].at[frm], left)

        def back_copy(self, j):
            to = high * LOW + lax.rem(low + j, LOW)
            return rcopy(self.out.at[low], self.out.at[low], self.sems[4].at[j], self.sems[5].at[low], to)

        def back_in(self, j):
            frm = lax.rem(low + j, LOW)
            return rcopy(self.out.at[frm], self.out.at[frm], self.sems[4].at[j], self.sems[5].at[frm], left)

        def start(self):
            for j in range(1, LOW):
                self.near_copy(j).start()
            self.near[low] = self.src[low]

        def middle(self):
            for j in range(1, LOW):
                self.near_in(j).wait_recv()
            tile = self.near[0]
            for l in range(1, LOW):
                tile = tile + self.near[l]
            self.far[high] = tile
            for j in range(1, n_high):
                self.far_copy(j).start()

        def back(self):
            for j in range(1, n_high):
                self.far_in(j).wait_recv()
            tile = self.far[0]
            for l in range(1, n_high):
                tile = tile + self.far[l]
            self.out[low] = tile
            for j in range(1, LOW):
                self.back_copy(j).start()

        def end(self):
            for j in range(1, LOW):
                self.back_in(j).wait_recv()

        def drain(self):
            for j in range(1, LOW):
                self.near_copy(j).wait_send()
                self.back_copy(j).wait_send()
            for j in range(1, n_high):
                self.far_copy(j).wait_send()

    soon = Exchange(early, early1, early2, early3, (e1s, e1r, e2s, e2r, e3s, e3r))
    later = Exchange(parts, big1, big2, fin, (b1s, b1r, b2s, b2r, b3s, b3r))

    class Apply:
        def __init__(self, kv, parts_ref, acc_ref):
            self.kv, self.zs, self.acc = kv, parts_ref, acc_ref

        def put(self, b, z):
            zh, zl = split(z)
            self.zs[b, 0:self.kv, :] = zh
            self.zs[b, self.kv:2 * self.kv, :] = zl

        def diag(self, b, z):
            self.acc[b] = onsite[b] * z

        def clear_tail(self):
            for t in range(HB):
                self.acc[rows + t] = jnp.zeros((self.kv, bs), F32)

        def product(self, z, hi, lo):
            part = mm(z, hi)
            return part[0:self.kv] + part[self.kv:] + mm(z[0:self.kv], lo)

        def onto(self, b):
            zb = self.zs[b]
            sums = [None] * (HB + 1)
            for s in range(SLOTS):
                moved = self.product(zb, bh[b * SLOTS + s], bl[b * SLOTS + s])
                off = offs[b * SLOTS + s]
                for o in range(HB + 1):
                    term = jnp.where(off == o, 1.0, 0.0) * moved
                    sums[o] = term if sums[o] is None else sums[o] + term
            for o in range(HB + 1):
                self.acc[b + o] = self.acc[b + o] + sums[o]

        def across(self, b):
            out = None
            for s in range(SLOTS):
                term = self.product(self.zs[b + offs[b * SLOTS + s]], th[b * SLOTS + s], tl[b * SLOTS + s])
                out = term if out is None else out + term
            self.acc[b] = self.acc[b] + out

        def halo_in(self, n):
            z_copy(n).wait_recv()
            for t in range(HB):
                self.put(rows + t, zhalo0[t] if n == 0 else zhalo[n - 1, t])

        def send_spill(self, n):
            for t in range(HB):
                if n == 0:
                    spill0[t] = self.acc[rows + t]
                else:
                    spill[n - 1, t] = self.acc[rows + t]
            spill_copy(n).start()

        def take_in(self, n):
            spill_copy(n).wait_recv()
            for t in range(HB):
                self.acc[t] = self.acc[t] + (inc0[t] if n == 0 else inc[n - 1, t])

    wide = Apply(2 * kvec, zsw, accw)
    thin = Apply(kvec, zs, acc)

    def precondition(x, b):
        dh, dl = split(x)
        part = mm(jnp.concatenate([dh, dl], axis=0), ph[b])
        return part[0:kvec] + part[kvec:] + mm(dh, plo[b])

    pltpu.make_async_copy(fw.at[:, pl.ds(0, kvec)], fw.at[:, pl.ds(0, kvec)], load_sem.at[0]).wait()
    for copy in smalls:
        copy.wait()
    for j in range(rows // SLOTS):
        precond_copy(j).wait()
        for t in range(SLOTS):
            b = j * SLOTS + t
            xh, xl = split(stage[j, t])
            ph[b] = xh.T
            plo[b] = xl.T
        block_copy(edge + j, j).start()
        for t in range(SLOTS):
            b = j * SLOTS + t
            v = fw[b, 0:kvec]
            fw[b, kvec:2 * kvec] = precondition(v, b)
            x = fw[b]
            wide.put(b, x)
            wide.diag(b, x)
    lax.fori_loop(0, rows, start_more, 0)
    wide.clear_tail()

    def take_row(b, slot):
        block_copy(b, slot).wait()
        for s in range(SLOTS):
            off = cols[s, b] - first - b
            off = jnp.where(off < 0, off + total, off)
            offs[b * SLOTS + s] = jnp.minimum(off, HB)
            alive = jnp.where(s < live[b], 1.0, 0.0)
            xh, xl = split(stage[slot, s] * alive)
            bh[b * SLOTS + s] = xh
            bl[b * SLOTS + s] = xl
            th[b * SLOTS + s] = xh.T
            tl[b * SLOTS + s] = xl.T

    def tail_row(i, c):
        take_row(edge + i, i)
        block_copy(i, i).start()
        wide.onto(edge + i)
        return c

    lax.fori_loop(0, HB, tail_row, 0)
    pl.semaphore_wait(barrier, n_greet)
    z_copy(0).start()
    wide.send_spill(0)

    def head_row(b, c):
        slot = lax.rem(b, STAGES)
        take_row(b, slot)

        @pl.when(b + STAGES < edge)
        def _():
            block_copy(b + STAGES, slot).start()

        wide.onto(b)
        wide.across(b)
        return c

    lax.fori_loop(0, edge, head_row, 0)
    wide.halo_in(0)
    for b in range(edge, rows):
        wide.across(b)
    wide.take_in(0)

    zero = jnp.zeros((kvec, bs), F32)

    def first_sums(b, c):
        x = fw[b, 0:kvec]
        im = accw[b, 0:kvec]
        fim[b] = im
        fhw[b] = accw[b, kvec:2 * kvec]
        return c[0] + x * im, c[1] + x * x

    num, den = lax.fori_loop(0, rows, first_sums, (zero, zero))
    total_of = lambda x: jnp.sum(x, axis=1, keepdims=True)
    red_start(0, total_of(num), total_of(den))

    pltpu.make_async_copy(fpv, fpv, load_sem.at[1]).wait()
    pltpu.make_async_copy(fpi, fpi, load_sem.at[2]).wait()

    def old_products(b, c):
        xh, xl = split(jnp.concatenate([fw[b, 0:kvec], fpv[b], fim[b], fpi[b]], axis=0))
        m = 2 * kvec
        part = mmt(jnp.concatenate([xh[0:m], xl[0:m]], axis=0), xh)
        return c + (part[0:m] + part[m:] + mmt(xh[0:m], xl))

    old = lax.fori_loop(0, rows, old_products, jnp.zeros((2 * kvec, 128), F32))
    for p in range(8):
        early[p] = old[8 * p:8 * p + 8]
    soon.start()

    for k in range(ITERS):
        n = k + 1
        field = fim if k == 0 else fa

        def prepare(b, field=field):
            z = precondition(field[b], b)
            fz[b] = z
            thin.put(b, z)
            thin.diag(b, z)

        for b in range(HB):
            prepare(b)
        z_copy(n).start()
        thin.clear_tail()
        for b in range(edge, rows):
            prepare(b)
        red_mid(k)
        for b in range(edge, rows):
            thin.onto(b)
        thin.send_spill(n)

        def interior(g, c, prepare=prepare):
            for t in range(4):
                prepare(4 + 4 * g + t)
            return c

        for g in range((edge - HB) // 4):
            interior(g, 0)
        (soon.middle, soon.back, soon.end)[k]()

        def body(g, c):
            for t in range(4):
                thin.onto(4 * g + t)
            for t in range(4):
                thin.across(4 * g + t)
            return c

        for g in range(edge // 4):
            body(g, 0)
        thin.halo_in(n)
        for b in range(edge, rows):
            thin.across(b)
        thin.take_in(n)
        z_copy(n).wait_send()
        top, bottom = red_end(k)
        if k == 0:
            qb[...] = jnp.broadcast_to(top / bottom, (kvec, bs))
        else:
            sb[...] = jnp.broadcast_to(top / (bottom + 1.0), (kvec, bs))

        def update(b, c, k=k):
            z, hz = fz[b], acc[b]
            q = qb[...]
            if k == 0:
                u = q * fw[b, kvec:2 * kvec] - z
                hu = q * fhw[b] - hz
                r = q * fw[b, 0:kvec] - fim[b]
                a = hu - q * u
                fu[b] = u
                fhu[b] = hu
                fr[b] = r
            else:
                m = hz - q * z
                s = sb[...]
                u, hu, a = fu[b], fhu[b], fa[b]
                r = fr[b] - s * a
                fr[b] = r
                if k == 1:
                    fc[b] = s * u
                    fh[b] = s * hu
                else:
                    fc[b] = fc[b] + s * u
                    fh[b] = fh[b] + s * hu
                a = a - s * m
                fu[b] = u - s * z
                fhu[b] = hu - s * hz
            fa[b] = a
            return c[0] + a * r, c[1] + a * a

        cross, own = lax.fori_loop(0, rows, update, (zero, zero))
        if k + 1 < ITERS:
            red_start(k + 1, total_of(cross), total_of(own))

    def put_out(b, c):
        at = pl.ds(pl.multiple_of(b * bs, bs), bs)
        pltpu.make_async_copy(fc.at[b], c_out.at[:, at], out_sem.at[0]).start()
        pltpu.make_async_copy(fu.at[b], u_out.at[:, at], out_sem.at[1]).start()
        return c

    red_start(ITERS, total_of(cross), total_of(own))
    lax.fori_loop(0, rows, put_out, 0)

    gram[...] = jnp.zeros_like(gram)

    def products(b, c):
        xh, xl = split(jnp.concatenate([fw[b, 0:kvec], fpv[b], fc[b], fu[b]], axis=0))
        yh, yl = split(jnp.concatenate([fim[b], fpi[b], fh[b], fhu[b]], axis=0))
        m = 2 * kvec
        left_side = jnp.concatenate([xh[m:], yh[m:], xl[m:], yl[m:]], axis=0)
        part = mmt(left_side, jnp.concatenate([xh, yh], axis=0))
        n = 2 * m
        gram[...] = gram[...] + (part[0:n] + part[n:] + mmt(left_side[0:n], jnp.concatenate([xl, yl], axis=0)))
        return c

    lax.fori_loop(0, rows, products, 0)
    hp = pltpu.roll(gram[2 * kvec:3 * kvec, 0:128], 64, 1)
    hup = pltpu.roll(gram[3 * kvec:4 * kvec, 0:128], 64, 1)
    last = span >= 3 * kvec
    quarters = (
        jnp.where(last, hp, gram[0:kvec, 0:128]),
        gram[kvec:2 * kvec, 0:128],
        jnp.where(last, hup, gram[0:kvec, 128:256]),
        gram[kvec:2 * kvec, 128:256],
    )
    for p in range(4):
        parts[2 * p] = quarters[p][0:kvec // 2]
        parts[2 * p + 1] = quarters[p][kvec // 2:]
    later.start()
    red_mid(ITERS)
    later.middle()
    top, bottom = red_end(ITERS)
    sums_out[...] = jnp.broadcast_to(top / (bottom + 1.0), (kvec, 128))
    later.back()
    for p in range(8):
        early_out[p] = early3[p]
    later.end()
    for p in range(8):
        late_out[p] = fin[p]
    pltpu.make_async_copy(fc, fc, out_sem.at[0]).wait()
    pltpu.make_async_copy(fu, fu, out_sem.at[1]).wait()

    soon.drain()
    later.drain()
    z_copy(0).wait_send()
    for n in range(ITERS + 1):
        spill_copy(n).wait_send()


def finish(kvec, c_in, u_in, early, late, step_in, corr, reduced, cbuf, ubuf, aug, sem):
    first = pltpu.make_async_copy(c_in, cbuf, sem.at[0])
    second = pltpu.make_async_copy(u_in, ubuf, sem.at[1])
    third = pltpu.make_async_copy(cbuf, corr, sem.at[2])
    first.start()
    second.start()
    step = step_in[:, 0:1]

    def add_last():
        wide = jnp.broadcast_to(step, (kvec, 512))
        first.wait()
        second.wait()

        def add(g, c):
            at = pl.ds(pl.multiple_of(g * 512, 512), 512)
            cbuf[:, at] = cbuf[:, at] + wide * ubuf[:, at]
            return c

        lax.fori_loop(0, cbuf.shape[1] // 512, add, 0)
        third.start()

    quarter = lambda p: jnp.concatenate([late[2 * p], late[2 * p + 1]], axis=0)
    half = lambda g: jnp.concatenate([early[4 * g + p] for p in range(4)], axis=0)
    full = reduce_basis([half(0), half(1)], [quarter(p) for p in range(4)], step, aug, kvec, add_last)
    reduced[...] = full[:, 0:3 * kvec]
    third.wait()


def local(n_dev, blocks, block_cols, live_counts, onsite_energy, precond, vectors, prev_vectors, prev_image):
    rows, slots, bs = blocks.shape[0], blocks.shape[1], blocks.shape[2]
    kvec = vectors.shape[0]
    n_high = n_dev // LOW
    field = pltpu.VMEM((rows, kvec, bs), F32)
    tiles = pltpu.VMEM((rows * slots, bs, bs), BF16)
    dma = pltpu.SemaphoreType.DMA
    hbm = pl.BlockSpec(memory_space=pl.ANY)
    vmem = pl.BlockSpec(memory_space=pltpu.VMEM)

    def run(*args):
        return kernel(n_dev, rows, kvec, bs, *args)

    outs = pl.pallas_call(
        run,
        out_shape=(
            jax.ShapeDtypeStruct(vectors.shape, F32),
            jax.ShapeDtypeStruct(vectors.shape, F32),
            jax.ShapeDtypeStruct((8, 8, 128), F32),
            jax.ShapeDtypeStruct((8, kvec // 2, 128), F32),
            jax.ShapeDtypeStruct((kvec, 128), F32),
        ),
        in_specs=[hbm] * 8,
        out_specs=(hbm, hbm, vmem, vmem, vmem),
        scratch_shapes=[
            pltpu.SMEM((slots, rows), jnp.int32),
            pltpu.SMEM((rows,), jnp.int32),
            pltpu.VMEM((rows, 1, bs), F32),
            pltpu.VMEM((STAGES, slots, bs, bs), F32),
            tiles, tiles, tiles, tiles,
            pltpu.VMEM((rows, bs, bs), BF16),
            pltpu.VMEM((rows, bs, bs), BF16),
            pltpu.SMEM((rows * slots,), jnp.int32),
            pltpu.VMEM((rows, 2 * kvec, bs), F32),
            field, field, field, field, field, field, field, field, field, field, field,
            pltpu.VMEM((rows + HB, 4 * kvec, bs), BF16),
            pltpu.VMEM((rows + HB, 2 * kvec, bs), F32),
            pltpu.VMEM((rows + HB, 2 * kvec, bs), BF16),
            pltpu.VMEM((rows + HB, kvec, bs), F32),
            pltpu.VMEM((kvec, bs), F32),
            pltpu.VMEM((kvec, bs), F32),
            pltpu.VMEM((ITERS, HB, kvec, bs), F32),
            pltpu.VMEM((ITERS, HB, kvec, bs), F32),
            pltpu.VMEM((ITERS, HB, kvec, bs), F32),
            pltpu.VMEM((HB, 2 * kvec, bs), F32),
            pltpu.VMEM((HB, 2 * kvec, bs), F32),
            pltpu.VMEM((HB, 2 * kvec, bs), F32),
            pltpu.VMEM((ITERS + 1, 2, 1, 128), F32),
            pltpu.VMEM((ITERS + 1, n_dev // 2, 1, 128), F32),
            pltpu.VMEM((4 * kvec, 256), F32),
            pltpu.VMEM((LOW, 8, 128), F32),
            pltpu.VMEM((LOW, 8, 128), F32),
            pltpu.VMEM((n_high, 8, 128), F32),
            pltpu.VMEM((LOW, 8, 128), F32),
            pltpu.VMEM((LOW, kvec // 2, 128), F32),
            pltpu.VMEM((LOW, kvec // 2, 128), F32),
            pltpu.VMEM((n_high, kvec // 2, 128), F32),
            pltpu.VMEM((LOW, kvec // 2, 128), F32),
            dma((STAGES,)), dma((6,)), dma((2,)),
            dma((ITERS + 1,)), dma((ITERS + 1,)), dma((ITERS + 1,)), dma((ITERS + 1,)),
            dma((ITERS + 1,)), dma((ITERS + 1,)), dma((ITERS + 1,)), dma((ITERS + 1,)),
            dma((LOW,)), dma((LOW,)), dma((n_high,)), dma((n_high,)), dma((LOW,)), dma((LOW,)),
            dma((LOW,)), dma((LOW,)), dma((n_high,)), dma((n_high,)), dma((LOW,)), dma((LOW,)),
        ],
        compiler_params=pltpu.CompilerParams(
            collective_id=0, has_side_effects=True, vmem_limit_bytes=63 * 1024 * 1024
        ),
    )(block_cols.T, live_counts, blocks, onsite_energy.reshape(rows, 1, bs), precond, vectors, prev_vectors, prev_image)

    def run_last(*args):
        return finish(kvec, *args)

    return pl.pallas_call(
        run_last,
        out_shape=(
            jax.ShapeDtypeStruct(vectors.shape, F32),
            jax.ShapeDtypeStruct((3 * kvec, 3 * kvec), F32),
        ),
        in_specs=[hbm, hbm, vmem, vmem, vmem],
        out_specs=(hbm, vmem),
        scratch_shapes=[
            pltpu.VMEM(vectors.shape, F32),
            pltpu.VMEM(vectors.shape, F32),
            pltpu.VMEM((3 * kvec, 256), F32),
            dma((3,)),
        ],
    )(*outs)


def solution(mesh):
    n_dev = mesh.shape["rows"]

    def step(*args):
        return local(n_dev, *args)

    return jax.shard_map(
        step,
        mesh=mesh,
        in_specs=(
            P("rows", None, None, None), P("rows", None), P("rows"), P("rows"),
            P("rows", None, None), P(None, "rows"), P(None, "rows"), P(None, "rows"),
        ),
        out_specs=(P(None, "rows"), P()),
        check_vma=False,
    )
```

```python
import jax
import jax.numpy as jnp
from jax import lax
from jax.experimental import pallas as pl
from jax.experimental.pallas import tpu as pltpu
from jax.sharding import PartitionSpec as P

MESH = pl.DeviceIdType.MESH
F32 = jnp.float32
BF16 = jnp.bfloat16
HB = 4
ITERS = 3
LOW = 8
SLOTS = 4
STAGES = 4


def split(x):
    high = x.astype(BF16)
    return high, (x - high.astype(F32)).astype(BF16)


def mm(a, b):
    return jnp.dot(a, b, preferred_element_type=F32)


def mmt(a, b):
    return lax.dot_general(a, b, (((1,), (1,)), ((), ())), preferred_element_type=F32)


def reduce_basis(early, late, step, aug, kvec, between):
    width = 128
    size = 3 * kvec
    lane = lax.broadcasted_iota(jnp.int32, (kvec, width), 1)
    row = lax.broadcasted_iota(jnp.int32, (kvec, width), 0)
    step_col = jnp.sum(jnp.where(lane == row + 2 * kvec, step, 0.0), axis=0, keepdims=True)
    rest = jnp.zeros((2 * kvec, width), F32)

    def turned(x):
        return jnp.concatenate([rest, x, jnp.zeros((kvec, width), F32)], axis=0).T

    lead = lane < 2 * kvec
    side = (lane >= 2 * kvec) & (lane < size)
    g_c, g_u, p_c, p_u = late
    mixed = g_c + step * g_u
    flip = turned(jnp.where(lead, mixed, g_u))
    square = mixed + step_col * (flip[2 * kvec:size] + step * pltpu.roll(g_u, width - kvec, 1))
    tail = jnp.where(side, square, jnp.where(lead, mixed, 0.0))
    for g in range(2):
        a = jnp.where(lead, early[g], jnp.where(side, flip[g * kvec:(g + 1) * kvec], 0.0))
        aug[g * kvec:(g + 1) * kvec, 0:width] = a + jnp.where(lane == row + g * kvec, 1.0, 0.0)
    aug[2 * kvec:size, 0:width] = tail + jnp.where(lane == row + 2 * kvec, 1.0, 0.0)
    for g in range(3):
        aug[g * kvec:(g + 1) * kvec, width:2 * width] = jnp.where(lane == row + g * kvec, 1.0, 0.0)
    mixed = p_c + step * p_u
    cross = pltpu.roll(g_c + step * p_c, 2 * kvec, 1)
    flip = turned(jnp.where(lane < kvec, mixed, jnp.where(lead, cross, p_u)))
    square = mixed + step_col * (flip[2 * kvec:size] + step * pltpu.roll(p_u, width - kvec, 1))
    x = []
    for g in range(2):
        moved = pltpu.roll(early[g], 2 * kvec, 1)
        x.append(jnp.where(lead, moved, jnp.where(side, flip[g * kvec:(g + 1) * kvec], 0.0)))
    x.append(jnp.where(side, square, jnp.where(lead, mixed, 0.0)))
    x = jnp.concatenate(x + [jnp.zeros((kvec, width), F32)], axis=0)

    sub = lax.broadcasted_iota(jnp.int32, (8, width), 0)
    for top in range(0, size, 8):
        if top == 2 * kvec:
            between()
        n = size - top
        cols = [jnp.broadcast_to(aug[top:size, top + c:top + c + 1], (n, width)) for c in range(8)]
        pivot_rows = aug[top:top + 8, :]
        facs = []
        for j in range(8):
            f = cols[j] * (1.0 / cols[j][j:j + 1, :])
            head = jnp.where(sub > j, f[0:8], 0.0)
            facs.append(f)
            for c in range(j + 1, 8):
                pr = cols[c][j:j + 1, :]
                new_head = cols[c][0:8] - head * pr
                cols[c] = new_head if n == 8 else jnp.concatenate([new_head, cols[c][8:] - f[8:] * pr], axis=0)
            both = jnp.concatenate([head, head], axis=1)
            pivot_rows = pivot_rows - both * pivot_rows[j:j + 1, :]
        aug[top:top + 8, :] = pivot_rows
        for r in range(top + 8, size, 8):
            block = aug[r:r + 8, :]
            for j in range(8):
                f = facs[j][r - top:r - top + 8]
                block = block - jnp.concatenate([f, f], axis=1) * pivot_rows[j:j + 1, :]
            aug[r:r + 8, :] = block

    at = lax.broadcasted_iota(jnp.int32, (size, width), 1)
    diagonal = jnp.where(at == lax.broadcasted_iota(jnp.int32, (size, width), 0), aug[:, 0:width], 0.0)
    by_row = lax.rsqrt(jnp.sum(diagonal, axis=1, keepdims=True))
    by_col = jnp.sum(diagonal, axis=0, keepdims=True)
    by_col = jnp.where(at[0:1] < size, lax.rsqrt(jnp.where(at[0:1] < size, by_col, 1.0)), 0.0)
    w = aug[:, width:2 * width]
    w_full = jnp.concatenate([w, jnp.zeros((kvec, width), F32)], axis=0)
    half = jnp.dot(w, x, precision=lax.Precision.HIGHEST, preferred_element_type=F32)
    full = lax.dot_general(half, w_full, (((1,), (1,)), ((), ())), precision=lax.Precision.HIGHEST, preferred_element_type=F32)
    return full * by_row * by_col


def kernel(
    n_dev, rows, kvec, bs,
    cols_in, live_in, blocks, onsite_in, precond, vec, pvec, pimg,
    c_out, u_out, early_out, late_out, sums_out,
    cols, live, onsite, stage, bh, bl, th, tl, ph, plo, offs,
    fw, fhw, fpv, fpi, fim, fr, fu, fhu, fa, fz, fc, fh, zsw, accw, zs, acc, qb, sb,
    zhalo, inc, spill, zhalo0, inc0, spill0, red1, red2, gram, early, early1, early2, early3, parts, big1, big2, fin,
    stage_sem, load_sem, out_sem, zs_sem, zr_sem, ss_sem, sr_sem,
    r1s, r1r, r2s, r2r, b1s, b1r, b2s, b2r, b3s, b3r, e1s, e1r, e2s, e2r, e3s, e3r,
):
    me = lax.axis_index("rows")
    low = lax.rem(me, LOW)
    high = lax.div(me, LOW)
    n_high = n_dev // LOW
    total = n_dev * rows
    first = me * rows
    right = lax.rem(me + 1, n_dev)
    left = lax.rem(me + n_dev - 1, n_dev)
    edge = rows - HB

    def field_copy(hbm, b):
        return hbm.at[:, pl.ds(b * bs, bs)]

    def block_copy(row, slot):
        return pltpu.make_async_copy(blocks.at[row], stage.at[slot], stage_sem.at[slot])

    def precond_copy(j):
        return pltpu.make_async_copy(precond.at[pl.ds(j * SLOTS, SLOTS)], stage.at[j], stage_sem.at[j])

    def start_loads(b, c):
        at = pl.ds(pl.multiple_of(b * bs, bs), bs)
        pltpu.make_async_copy(vec.at[:, at], fw.at[b, pl.ds(0, kvec)], load_sem.at[0]).start()
        return c

    smalls = [
        pltpu.make_async_copy(x, y, load_sem.at[3 + t])
        for t, (x, y) in enumerate(((cols_in, cols), (live_in, live), (onsite_in, onsite)))
    ]
    lax.fori_loop(0, rows, start_loads, 0)
    for j in range(STAGES):
        precond_copy(j).start()
    for copy in smalls:
        copy.start()

    barrier = pltpu.get_barrier_semaphore()
    others = n_dev // 2

    def greet(j, c):
        pl.semaphore_signal(barrier, inc=1, device_id=(lax.rem(me + 2 * j, n_dev),), device_id_type=MESH)
        return c

    lax.fori_loop(1, others, greet, 0)
    partner = me + 1 - 2 * lax.rem(me, 2)
    near_odd = [high * LOW + lax.rem(low + j, LOW) for j in range(1, LOW, 2)]
    for peer in [left, right] + near_odd:
        pl.semaphore_signal(barrier, inc=1, device_id=(peer,), device_id_type=MESH)
    n_greet = others - 1 + 2 + len(near_odd)

    def start_more(b, c):
        at = pl.ds(pl.multiple_of(b * bs, bs), bs)
        pltpu.make_async_copy(pvec.at[:, at], fpv.at[b], load_sem.at[1]).start()
        pltpu.make_async_copy(pimg.at[:, at], fpi.at[b], load_sem.at[2]).start()
        return c

    def rcopy(src, dst, s_sem, r_sem, to):
        return pltpu.make_async_remote_copy(
            src_ref=src, dst_ref=dst, send_sem=s_sem, recv_sem=r_sem,
            device_id=(to,), device_id_type=MESH,
        )

    def z_copy(n):
        src, dst = (fw, zhalo0) if n == 0 else (fz, zhalo.at[n - 1])
        return rcopy(src.at[pl.ds(0, HB)], dst, zs_sem.at[n], zr_sem.at[n], left)

    def spill_copy(n):
        src, dst = (spill0, inc0) if n == 0 else (spill.at[n - 1], inc.at[n - 1])
        return rcopy(src, dst, ss_sem.at[n], sr_sem.at[n], right)

    def pair_copy(i):
        return rcopy(red1.at[i, 0], red1.at[i, 1], r1s.at[i], r1r.at[i], partner)

    def chip_copy(i, j):
        at = red2.at[i, lax.div(me, 2)]
        return rcopy(at, at, r2s.at[i], r2r.at[i], lax.rem(me + 2 * j, n_dev))

    span = lax.broadcasted_iota(jnp.int32, (kvec, 128), 1)
    rank = lax.broadcasted_iota(jnp.int32, (kvec, 128), 0)

    def red_start(i, a, b):
        both = jnp.where(span == rank, a, 0.0) + jnp.where(span == rank + kvec, b, 0.0)
        red1[i, 0] = jnp.sum(both, axis=0, keepdims=True)
        pair_copy(i).start()

    def red_mid(i):
        pair_copy(i).wait_recv()
        red2[i, lax.div(me, 2)] = red1[i, 0] + red1[i, 1]

        for j in range(1, others):
            chip_copy(i, j).start()

    def red_end(i):
        got = red2.at[i, pl.ds(0, others - 1)]
        pltpu.make_async_copy(got, got, r2r.at[i]).wait()
        pltpu.make_async_copy(got, got, r2s.at[i]).wait()
        pair_copy(i).wait_send()
        line = jnp.broadcast_to(jnp.sum(red2[i], axis=0), (kvec, 128))
        top = jnp.sum(jnp.where(span == rank, line, 0.0), axis=1, keepdims=True)
        bottom = jnp.sum(jnp.where(span == rank + kvec, line, 0.0), axis=1, keepdims=True)
        return top, bottom

    class Exchange:
        def __init__(self, src, near, far, out, sems):
            self.src, self.near, self.far, self.out, self.sems = src, near, far, out, sems

        def near_copy(self, j):
            to = lax.rem(low + j, LOW)
            return rcopy(self.src.at[to], self.near.at[low], self.sems[0].at[j], self.sems[1].at[low], high * LOW + to)

        def near_in(self, j):
            frm = lax.rem(low + j, LOW)
            return rcopy(self.src.at[frm], self.near.at[frm], self.sems[0].at[j], self.sems[1].at[frm], left)

        def far_copy(self, j):
            to = lax.rem(high + j, n_high) * LOW + low
            return rcopy(self.far.at[high], self.far.at[high], self.sems[2].at[j], self.sems[3].at[high], to)

        def far_in(self, j):
            frm = lax.rem(high + j, n_high)
            return rcopy(self.far.at[frm], self.far.at[frm], self.sems[2].at[j], self.sems[3].at[frm], left)

        def back_copy(self, j):
            to = high * LOW + lax.rem(low + j, LOW)
            return rcopy(self.out.at[low], self.out.at[low], self.sems[4].at[j], self.sems[5].at[low], to)

        def back_in(self, j):
            frm = lax.rem(low + j, LOW)
            return rcopy(self.out.at[frm], self.out.at[frm], self.sems[4].at[j], self.sems[5].at[frm], left)

        def start(self):
            for j in range(1, LOW):
                self.near_copy(j).start()
            self.near[low] = self.src[low]

        def middle(self):
            for j in range(1, LOW):
                self.near_in(j).wait_recv()
            tile = self.near[0]
            for l in range(1, LOW):
                tile = tile + self.near[l]
            self.far[high] = tile
            for j in range(1, n_high):
                self.far_copy(j).start()

        def back(self):
            for j in range(1, n_high):
                self.far_in(j).wait_recv()
            tile = self.far[0]
            for l in range(1, n_high):
                tile = tile + self.far[l]
            self.out[low] = tile
            for j in range(1, LOW):
                self.back_copy(j).start()

        def end(self):
            for j in range(1, LOW):
                self.back_in(j).wait_recv()

        def drain(self):
            for j in range(1, LOW):
                self.near_copy(j).wait_send()
                self.back_copy(j).wait_send()
            for j in range(1, n_high):
                self.far_copy(j).wait_send()

    soon = Exchange(early, early1, early2, early3, (e1s, e1r, e2s, e2r, e3s, e3r))
    later = Exchange(parts, big1, big2, fin, (b1s, b1r, b2s, b2r, b3s, b3r))

    class Apply:
        def __init__(self, kv, parts_ref, acc_ref):
            self.kv, self.zs, self.acc = kv, parts_ref, acc_ref

        def put(self, b, z):
            zh, zl = split(z)
            self.zs[b, 0:self.kv, :] = zh
            self.zs[b, self.kv:2 * self.kv, :] = zl

        def diag(self, b, z):
            self.acc[b] = onsite[b] * z

        def clear_tail(self):
            for t in range(HB):
                self.acc[rows + t] = jnp.zeros((self.kv, bs), F32)

        def product(self, z, hi, lo):
            part = mm(z, hi)
            return part[0:self.kv] + part[self.kv:] + mm(z[0:self.kv], lo)

        def onto(self, b):
            zb = self.zs[b]
            sums = [None] * (HB + 1)
            for s in range(SLOTS):
                moved = self.product(zb, bh[b * SLOTS + s], bl[b * SLOTS + s])
                off = offs[b * SLOTS + s]
                for o in range(HB + 1):
                    term = jnp.where(off == o, 1.0, 0.0) * moved
                    sums[o] = term if sums[o] is None else sums[o] + term
            for o in range(HB + 1):
                self.acc[b + o] = self.acc[b + o] + sums[o]

        def across(self, b):
            out = None
            for s in range(SLOTS):
                term = self.product(self.zs[b + offs[b * SLOTS + s]], th[b * SLOTS + s], tl[b * SLOTS + s])
                out = term if out is None else out + term
            self.acc[b] = self.acc[b] + out

        def halo_in(self, n):
            z_copy(n).wait_recv()
            for t in range(HB):
                self.put(rows + t, zhalo0[t] if n == 0 else zhalo[n - 1, t])

        def send_spill(self, n):
            for t in range(HB):
                if n == 0:
                    spill0[t] = self.acc[rows + t]
                else:
                    spill[n - 1, t] = self.acc[rows + t]
            spill_copy(n).start()

        def take_in(self, n):
            spill_copy(n).wait_recv()
            for t in range(HB):
                self.acc[t] = self.acc[t] + (inc0[t] if n == 0 else inc[n - 1, t])

    wide = Apply(2 * kvec, zsw, accw)
    thin = Apply(kvec, zs, acc)

    def precondition(x, b):
        dh, dl = split(x)
        part = mm(jnp.concatenate([dh, dl], axis=0), ph[b])
        return part[0:kvec] + part[kvec:] + mm(dh, plo[b])

    pltpu.make_async_copy(fw.at[:, pl.ds(0, kvec)], fw.at[:, pl.ds(0, kvec)], load_sem.at[0]).wait()
    for copy in smalls:
        copy.wait()
    for j in range(rows // SLOTS):
        precond_copy(j).wait()
        for t in range(SLOTS):
            b = j * SLOTS + t
            xh, xl = split(stage[j, t])
            ph[b] = xh.T
            plo[b] = xl.T
        block_copy(edge + j, j).start()
        for t in range(SLOTS):
            b = j * SLOTS + t
            v = fw[b, 0:kvec]
            fw[b, kvec:2 * kvec] = precondition(v, b)
            x = fw[b]
            wide.put(b, x)
            wide.diag(b, x)
    lax.fori_loop(0, rows, start_more, 0)
    wide.clear_tail()

    def take_row(b, slot):
        block_copy(b, slot).wait()
        for s in range(SLOTS):
            off = cols[s, b] - first - b
            off = jnp.where(off < 0, off + total, off)
            offs[b * SLOTS + s] = jnp.minimum(off, HB)
            alive = jnp.where(s < live[b], 1.0, 0.0)
            xh, xl = split(stage[slot, s] * alive)
            bh[b * SLOTS + s] = xh
            bl[b * SLOTS + s] = xl
            th[b * SLOTS + s] = bh[b * SLOTS + s].T
            tl[b * SLOTS + s] = bl[b * SLOTS + s].T

    def tail_row(i, c):
        take_row(edge + i, i)
        block_copy(i, i).start()
        wide.onto(edge + i)
        return c

    lax.fori_loop(0, HB, tail_row, 0)
    pl.semaphore_wait(barrier, n_greet)
    z_copy(0).start()
    wide.send_spill(0)

    def head_row(b, c):
        slot = lax.rem(b, STAGES)
        take_row(b, slot)

        @pl.when(b + STAGES < edge)
        def _():
            block_copy(b + STAGES, slot).start()

        wide.onto(b)
        wide.across(b)
        return c

    lax.fori_loop(0, edge, head_row, 0)
    wide.halo_in(0)
    for b in range(edge, rows):
        wide.across(b)
    wide.take_in(0)

    zero = jnp.zeros((kvec, bs), F32)

    def first_sums(b, c):
        x = fw[b, 0:kvec]
        im = accw[b, 0:kvec]
        fim[b] = im
        fhw[b] = accw[b, kvec:2 * kvec]
        return c[0] + x * im, c[1] + x * x

    num, den = lax.fori_loop(0, rows, first_sums, (zero, zero))
    total_of = lambda x: jnp.sum(x, axis=1, keepdims=True)
    red_start(0, total_of(num), total_of(den))

    pltpu.make_async_copy(fpv, fpv, load_sem.at[1]).wait()
    pltpu.make_async_copy(fpi, fpi, load_sem.at[2]).wait()

    def old_products(b, c):
        xh, xl = split(jnp.concatenate([fw[b, 0:kvec], fpv[b], fim[b], fpi[b]], axis=0))
        m = 2 * kvec
        part = mmt(jnp.concatenate([xh[0:m], xl[0:m]], axis=0), xh)
        return c + (part[0:m] + part[m:] + mmt(xh[0:m], xl))

    old = lax.fori_loop(0, rows, old_products, jnp.zeros((2 * kvec, 128), F32))
    for p in range(8):
        early[p] = old[8 * p:8 * p + 8]
    soon.start()

    for k in range(ITERS):
        n = k + 1
        field = fim if k == 0 else fa

        def prepare(b, field=field):
            z = precondition(field[b], b)
            fz[b] = z
            thin.put(b, z)
            thin.diag(b, z)

        for b in range(HB):
            prepare(b)
        z_copy(n).start()
        thin.clear_tail()
        for b in range(edge, rows):
            prepare(b)
        red_mid(k)
        for b in range(edge, rows):
            thin.onto(b)
        thin.send_spill(n)

        def interior(g, c, prepare=prepare):
            for t in range(4):
                prepare(4 + 4 * g + t)
            return c

        for g in range((edge - HB) // 4):
            interior(g, 0)

        def body(g, c):
            for t in range(4):
                thin.onto(4 * g + t)
            for t in range(4):
                thin.across(4 * g + t)
            return c

        for g in range(edge // 4):
            body(g, 0)
        thin.halo_in(n)
        for b in range(edge, rows):
            thin.across(b)
        thin.take_in(n)
        z_copy(n).wait_send()
        (soon.middle, soon.back, soon.end)[k]()
        top, bottom = red_end(k)
        if k == 0:
            qb[...] = jnp.broadcast_to(top / bottom, (kvec, bs))
        else:
            sb[...] = jnp.broadcast_to(top / (bottom + 1.0), (kvec, bs))

        def update(b, c, k=k):
            z, hz = fz[b], acc[b]
            q = qb[...]
            if k == 0:
                u = q * fw[b, kvec:2 * kvec] - z
                hu = q * fhw[b] - hz
                r = q * fw[b, 0:kvec] - fim[b]
                a = hu - q * u
                fu[b] = u
                fhu[b] = hu
                fr[b] = r
            else:
                m = hz - q * z
                s = sb[...]
                u, hu, a = fu[b], fhu[b], fa[b]
                r = fr[b] - s * a
                fr[b] = r
                if k == 1:
                    fc[b] = s * u
                    fh[b] = s * hu
                else:
                    fc[b] = fc[b] + s * u
                    fh[b] = fh[b] + s * hu
                a = a - s * m
                fu[b] = u - s * z
                fhu[b] = hu - s * hz
            fa[b] = a
            return c[0] + a * r, c[1] + a * a

        cross, own = lax.fori_loop(0, rows, update, (zero, zero))
        if k + 1 < ITERS:
            red_start(k + 1, total_of(cross), total_of(own))

    def put_out(b, c):
        at = pl.ds(pl.multiple_of(b * bs, bs), bs)
        pltpu.make_async_copy(fc.at[b], c_out.at[:, at], out_sem.at[0]).start()
        pltpu.make_async_copy(fu.at[b], u_out.at[:, at], out_sem.at[1]).start()
        return c

    red_start(ITERS, total_of(cross), total_of(own))
    lax.fori_loop(0, rows, put_out, 0)

    def product_of(b):
        xh, xl = split(jnp.concatenate([fw[b, 0:kvec], fpv[b], fc[b], fu[b]], axis=0))
        yh, yl = split(jnp.concatenate([fim[b], fpi[b], fh[b], fhu[b]], axis=0))
        m = 2 * kvec
        n = 2 * m
        left_side = jnp.concatenate([xh[m:], yh[m:], xl[m:], yl[m:]], axis=0)
        part = mmt(left_side, jnp.concatenate([xh, yh], axis=0))
        return part[0:n], part[n:], mmt(left_side[0:n], jnp.concatenate([xl, yl], axis=0))

    gram[...] = jnp.zeros_like(gram)

    def products(g, c):
        one, two = product_of(2 * g), product_of(2 * g + 1)
        gram[...] = gram[...] + ((one[0] + two[0]) + (one[1] + two[1]) + (one[2] + two[2]))
        return c

    lax.fori_loop(0, rows // 2, products, 0)
    hp = pltpu.roll(gram[2 * kvec:3 * kvec, 0:128], 64, 1)
    hup = pltpu.roll(gram[3 * kvec:4 * kvec, 0:128], 64, 1)
    last = span >= 3 * kvec
    quarters = (
        jnp.where(last, hp, gram[0:kvec, 0:128]),
        gram[kvec:2 * kvec, 0:128],
        jnp.where(last, hup, gram[0:kvec, 128:256]),
        gram[kvec:2 * kvec, 128:256],
    )
    for p in range(4):
        parts[2 * p] = quarters[p][0:kvec // 2]
        parts[2 * p + 1] = quarters[p][kvec // 2:]
    later.start()
    red_mid(ITERS)
    later.middle()
    top, bottom = red_end(ITERS)
    sums_out[...] = jnp.broadcast_to(top / (bottom + 1.0), (kvec, 128))
    later.back()
    for p in range(8):
        early_out[p] = early3[p]
    later.end()
    for p in range(8):
        late_out[p] = fin[p]
    pltpu.make_async_copy(fc, fc, out_sem.at[0]).wait()
    pltpu.make_async_copy(fu, fu, out_sem.at[1]).wait()

    soon.drain()
    later.drain()
    z_copy(0).wait_send()
    for n in range(ITERS + 1):
        spill_copy(n).wait_send()


def finish(kvec, c_in, u_in, early, late, step_in, corr, reduced, cbuf, ubuf, aug, sem):
    first = pltpu.make_async_copy(c_in, cbuf, sem.at[0])
    second = pltpu.make_async_copy(u_in, ubuf, sem.at[1])
    third = pltpu.make_async_copy(cbuf, corr, sem.at[2])
    first.start()
    second.start()
    step = step_in[:, 0:1]

    def add_last():
        wide = jnp.broadcast_to(step, (kvec, 512))
        first.wait()
        second.wait()

        def add(g, c):
            at = pl.ds(pl.multiple_of(g * 512, 512), 512)
            cbuf[:, at] = cbuf[:, at] + wide * ubuf[:, at]
            return c

        lax.fori_loop(0, cbuf.shape[1] // 512, add, 0)
        third.start()

    quarter = lambda p: jnp.concatenate([late[2 * p], late[2 * p + 1]], axis=0)
    half = lambda g: jnp.concatenate([early[4 * g + p] for p in range(4)], axis=0)
    full = reduce_basis([half(0), half(1)], [quarter(p) for p in range(4)], step, aug, kvec, add_last)
    reduced[...] = full[:, 0:3 * kvec]
    third.wait()


def local(n_dev, blocks, block_cols, live_counts, onsite_energy, precond, vectors, prev_vectors, prev_image):
    rows, slots, bs = blocks.shape[0], blocks.shape[1], blocks.shape[2]
    kvec = vectors.shape[0]
    n_high = n_dev // LOW
    field = pltpu.VMEM((rows, kvec, bs), F32)
    tiles = pltpu.VMEM((rows * slots, bs, bs), BF16)
    dma = pltpu.SemaphoreType.DMA
    hbm = pl.BlockSpec(memory_space=pl.ANY)
    vmem = pl.BlockSpec(memory_space=pltpu.VMEM)

    def run(*args):
        return kernel(n_dev, rows, kvec, bs, *args)

    outs = pl.pallas_call(
        run,
        out_shape=(
            jax.ShapeDtypeStruct(vectors.shape, F32),
            jax.ShapeDtypeStruct(vectors.shape, F32),
            jax.ShapeDtypeStruct((8, 8, 128), F32),
            jax.ShapeDtypeStruct((8, kvec // 2, 128), F32),
            jax.ShapeDtypeStruct((kvec, 128), F32),
        ),
        in_specs=[hbm] * 8,
        out_specs=(hbm, hbm, vmem, vmem, vmem),
        scratch_shapes=[
            pltpu.SMEM((slots, rows), jnp.int32),
            pltpu.SMEM((rows,), jnp.int32),
            pltpu.VMEM((rows, 1, bs), F32),
            pltpu.VMEM((STAGES, slots, bs, bs), F32),
            tiles, tiles, tiles, tiles,
            pltpu.VMEM((rows, bs, bs), BF16),
            pltpu.VMEM((rows, bs, bs), BF16),
            pltpu.SMEM((rows * slots,), jnp.int32),
            pltpu.VMEM((rows, 2 * kvec, bs), F32),
            field, field, field, field, field, field, field, field, field, field, field,
            pltpu.VMEM((rows + HB, 4 * kvec, bs), BF16),
            pltpu.VMEM((rows + HB, 2 * kvec, bs), F32),
            pltpu.VMEM((rows + HB, 2 * kvec, bs), BF16),
            pltpu.VMEM((rows + HB, kvec, bs), F32),
            pltpu.VMEM((kvec, bs), F32),
            pltpu.VMEM((kvec, bs), F32),
            pltpu.VMEM((ITERS, HB, kvec, bs), F32),
            pltpu.VMEM((ITERS, HB, kvec, bs), F32),
            pltpu.VMEM((ITERS, HB, kvec, bs), F32),
            pltpu.VMEM((HB, 2 * kvec, bs), F32),
            pltpu.VMEM((HB, 2 * kvec, bs), F32),
            pltpu.VMEM((HB, 2 * kvec, bs), F32),
            pltpu.VMEM((ITERS + 1, 2, 1, 128), F32),
            pltpu.VMEM((ITERS + 1, n_dev // 2, 1, 128), F32),
            pltpu.VMEM((4 * kvec, 256), F32),
            pltpu.VMEM((LOW, 8, 128), F32),
            pltpu.VMEM((LOW, 8, 128), F32),
            pltpu.VMEM((n_high, 8, 128), F32),
            pltpu.VMEM((LOW, 8, 128), F32),
            pltpu.VMEM((LOW, kvec // 2, 128), F32),
            pltpu.VMEM((LOW, kvec // 2, 128), F32),
            pltpu.VMEM((n_high, kvec // 2, 128), F32),
            pltpu.VMEM((LOW, kvec // 2, 128), F32),
            dma((STAGES,)), dma((6,)), dma((2,)),
            dma((ITERS + 1,)), dma((ITERS + 1,)), dma((ITERS + 1,)), dma((ITERS + 1,)),
            dma((ITERS + 1,)), dma((ITERS + 1,)), dma((ITERS + 1,)), dma((ITERS + 1,)),
            dma((LOW,)), dma((LOW,)), dma((n_high,)), dma((n_high,)), dma((LOW,)), dma((LOW,)),
            dma((LOW,)), dma((LOW,)), dma((n_high,)), dma((n_high,)), dma((LOW,)), dma((LOW,)),
        ],
        compiler_params=pltpu.CompilerParams(
            collective_id=0, has_side_effects=True, vmem_limit_bytes=63 * 1024 * 1024
        ),
    )(block_cols.T, live_counts, blocks, onsite_energy.reshape(rows, 1, bs), precond, vectors, prev_vectors, prev_image)

    def run_last(*args):
        return finish(kvec, *args)

    return pl.pallas_call(
        run_last,
        out_shape=(
            jax.ShapeDtypeStruct(vectors.shape, F32),
            jax.ShapeDtypeStruct((3 * kvec, 3 * kvec), F32),
        ),
        in_specs=[hbm, hbm, vmem, vmem, vmem],
        out_specs=(hbm, vmem),
        scratch_shapes=[
            pltpu.VMEM(vectors.shape, F32),
            pltpu.VMEM(vectors.shape, F32),
            pltpu.VMEM((3 * kvec, 256), F32),
            dma((3,)),
        ],
    )(*outs)


def solution(mesh):
    n_dev = mesh.shape["rows"]

    def step(*args):
        return local(n_dev, *args)

    return jax.shard_map(
        step,
        mesh=mesh,
        in_specs=(
            P("rows", None, None, None), P("rows", None), P("rows"), P("rows"),
            P("rows", None, None), P(None, "rows"), P(None, "rows"), P(None, "rows"),
        ),
        out_specs=(P(None, "rows"), P()),
        check_vma=False,
    )
```

```python
import jax
import jax.numpy as jnp
from jax import lax
from jax.experimental import pallas as pl
from jax.experimental.pallas import tpu as pltpu
from jax.sharding import PartitionSpec as P

MESH = pl.DeviceIdType.MESH
F32 = jnp.float32
BF16 = jnp.bfloat16
HB = 4
ITERS = 3
LOW = 8
SLOTS = 4
STAGES = 4


def split(x):
    high = x.astype(BF16)
    return high, (x - high.astype(F32)).astype(BF16)


def mm(a, b):
    return jnp.dot(a, b, preferred_element_type=F32)


def mmt(a, b):
    return lax.dot_general(a, b, (((1,), (1,)), ((), ())), preferred_element_type=F32)


def reduce_basis(early, late, step, aug, kvec, between):
    width = 128
    size = 3 * kvec
    lane = lax.broadcasted_iota(jnp.int32, (kvec, width), 1)
    row = lax.broadcasted_iota(jnp.int32, (kvec, width), 0)
    step_col = jnp.sum(jnp.where(lane == row + 2 * kvec, step, 0.0), axis=0, keepdims=True)
    rest = jnp.zeros((2 * kvec, width), F32)

    def turned(x):
        return jnp.concatenate([rest, x, jnp.zeros((kvec, width), F32)], axis=0).T

    lead = lane < 2 * kvec
    side = (lane >= 2 * kvec) & (lane < size)
    g_c, g_u, p_c, p_u = late
    mixed = g_c + step * g_u
    flip = turned(jnp.where(lead, mixed, g_u))
    square = mixed + step_col * (flip[2 * kvec:size] + step * pltpu.roll(g_u, width - kvec, 1))
    tail = jnp.where(side, square, jnp.where(lead, mixed, 0.0))
    for g in range(2):
        a = jnp.where(lead, early[g], jnp.where(side, flip[g * kvec:(g + 1) * kvec], 0.0))
        aug[g * kvec:(g + 1) * kvec, 0:width] = a + jnp.where(lane == row + g * kvec, 1.0, 0.0)
    aug[2 * kvec:size, 0:width] = tail + jnp.where(lane == row + 2 * kvec, 1.0, 0.0)
    for g in range(3):
        aug[g * kvec:(g + 1) * kvec, width:2 * width] = jnp.where(lane == row + g * kvec, 1.0, 0.0)
    mixed = p_c + step * p_u
    cross = pltpu.roll(g_c + step * p_c, 2 * kvec, 1)
    flip = turned(jnp.where(lane < kvec, mixed, jnp.where(lead, cross, p_u)))
    square = mixed + step_col * (flip[2 * kvec:size] + step * pltpu.roll(p_u, width - kvec, 1))
    x = []
    for g in range(2):
        moved = pltpu.roll(early[g], 2 * kvec, 1)
        x.append(jnp.where(lead, moved, jnp.where(side, flip[g * kvec:(g + 1) * kvec], 0.0)))
    x.append(jnp.where(side, square, jnp.where(lead, mixed, 0.0)))
    x = jnp.concatenate(x + [jnp.zeros((kvec, width), F32)], axis=0)

    sub = lax.broadcasted_iota(jnp.int32, (8, width), 0)
    for top in range(0, size, 8):
        if top == 2 * kvec:
            between()
        n = size - top
        cols = [jnp.broadcast_to(aug[top:size, top + c:top + c + 1], (n, width)) for c in range(8)]
        pivot_rows = aug[top:top + 8, :]
        facs = []
        for j in range(8):
            f = cols[j] * (1.0 / cols[j][j:j + 1, :])
            head = jnp.where(sub > j, f[0:8], 0.0)
            facs.append(f)
            for c in range(j + 1, 8):
                pr = cols[c][j:j + 1, :]
                new_head = cols[c][0:8] - head * pr
                cols[c] = new_head if n == 8 else jnp.concatenate([new_head, cols[c][8:] - f[8:] * pr], axis=0)
            both = jnp.concatenate([head, head], axis=1)
            pivot_rows = pivot_rows - both * pivot_rows[j:j + 1, :]
        aug[top:top + 8, :] = pivot_rows
        for r in range(top + 8, size, 8):
            block = aug[r:r + 8, :]
            for j in range(8):
                f = facs[j][r - top:r - top + 8]
                block = block - jnp.concatenate([f, f], axis=1) * pivot_rows[j:j + 1, :]
            aug[r:r + 8, :] = block

    at = lax.broadcasted_iota(jnp.int32, (size, width), 1)
    diagonal = jnp.where(at == lax.broadcasted_iota(jnp.int32, (size, width), 0), aug[:, 0:width], 0.0)
    by_row = lax.rsqrt(jnp.sum(diagonal, axis=1, keepdims=True))
    by_col = jnp.sum(diagonal, axis=0, keepdims=True)
    by_col = jnp.where(at[0:1] < size, lax.rsqrt(jnp.where(at[0:1] < size, by_col, 1.0)), 0.0)
    w = aug[:, width:2 * width]
    w_full = jnp.concatenate([w, jnp.zeros((kvec, width), F32)], axis=0)
    half = jnp.dot(w, x, precision=lax.Precision.HIGHEST, preferred_element_type=F32)
    full = lax.dot_general(half, w_full, (((1,), (1,)), ((), ())), precision=lax.Precision.HIGHEST, preferred_element_type=F32)
    return full * by_row * by_col


def kernel(
    n_dev, rows, kvec, bs,
    cols_in, live_in, blocks, onsite_in, precond, vec, pvec, pimg,
    c_out, u_out, early_out, late_out, sums_out,
    cols, live, onsite, stage, bh, bl, th, tl, ph, plo, offs,
    fw, fhw, fpv, fpi, fim, fr, fu, fhu, fa, fz, fc, fh, zsw, accw, zs, acc, qb, sb,
    zhalo, inc, spill, zhalo0, inc0, spill0, red1, red2, gram, early, early1, early2, early3, parts, big1, big2, fin,
    stage_sem, load_sem, out_sem, zs_sem, zr_sem, ss_sem, sr_sem,
    r1s, r1r, r2s, r2r, b1s, b1r, b2s, b2r, b3s, b3r, e1s, e1r, e2s, e2r, e3s, e3r,
):
    me = lax.axis_index("rows")
    low = lax.rem(me, LOW)
    high = lax.div(me, LOW)
    n_high = n_dev // LOW
    total = n_dev * rows
    first = me * rows
    right = lax.rem(me + 1, n_dev)
    left = lax.rem(me + n_dev - 1, n_dev)
    edge = rows - HB

    def field_copy(hbm, b):
        return hbm.at[:, pl.ds(b * bs, bs)]

    def block_copy(row, slot):
        return pltpu.make_async_copy(blocks.at[row], stage.at[slot], stage_sem.at[slot])

    def precond_copy(j):
        return pltpu.make_async_copy(precond.at[pl.ds(j * SLOTS, SLOTS)], stage.at[j], stage_sem.at[j])

    def start_loads(b, c):
        at = pl.ds(pl.multiple_of(b * bs, bs), bs)
        pltpu.make_async_copy(vec.at[:, at], fw.at[b, pl.ds(0, kvec)], load_sem.at[0]).start()
        return c

    smalls = [
        pltpu.make_async_copy(x, y, load_sem.at[3 + t])
        for t, (x, y) in enumerate(((cols_in, cols), (live_in, live), (onsite_in, onsite)))
    ]
    lax.fori_loop(0, rows, start_loads, 0)
    for j in range(STAGES):
        precond_copy(j).start()
    for copy in smalls:
        copy.start()

    barrier = pltpu.get_barrier_semaphore()
    others = n_dev // 2

    def greet(j, c):
        pl.semaphore_signal(barrier, inc=1, device_id=(lax.rem(me + 2 * j, n_dev),), device_id_type=MESH)
        return c

    lax.fori_loop(1, others, greet, 0)
    partner = me + 1 - 2 * lax.rem(me, 2)
    near_odd = [high * LOW + lax.rem(low + j, LOW) for j in range(1, LOW, 2)]
    for peer in [left, right] + near_odd:
        pl.semaphore_signal(barrier, inc=1, device_id=(peer,), device_id_type=MESH)
    n_greet = others - 1 + 2 + len(near_odd)

    def start_more(b, c):
        at = pl.ds(pl.multiple_of(b * bs, bs), bs)
        pltpu.make_async_copy(pvec.at[:, at], fpv.at[b], load_sem.at[1]).start()
        pltpu.make_async_copy(pimg.at[:, at], fpi.at[b], load_sem.at[2]).start()
        return c

    def rcopy(src, dst, s_sem, r_sem, to):
        return pltpu.make_async_remote_copy(
            src_ref=src, dst_ref=dst, send_sem=s_sem, recv_sem=r_sem,
            device_id=(to,), device_id_type=MESH,
        )

    def z_copy(n):
        src, dst = (fw, zhalo0) if n == 0 else (fz, zhalo.at[n - 1])
        return rcopy(src.at[pl.ds(0, HB)], dst, zs_sem.at[n], zr_sem.at[n], left)

    def spill_copy(n):
        src, dst = (spill0, inc0) if n == 0 else (spill.at[n - 1], inc.at[n - 1])
        return rcopy(src, dst, ss_sem.at[n], sr_sem.at[n], right)

    def pair_copy(i):
        return rcopy(red1.at[i, 0], red1.at[i, 1], r1s.at[i], r1r.at[i], partner)

    def chip_copy(i, j):
        at = red2.at[i, lax.div(me, 2)]
        return rcopy(at, at, r2s.at[i], r2r.at[i], lax.rem(me + 2 * j, n_dev))

    span = lax.broadcasted_iota(jnp.int32, (kvec, 128), 1)
    rank = lax.broadcasted_iota(jnp.int32, (kvec, 128), 0)

    def red_start(i, a, b):
        both = jnp.where(span == rank, a, 0.0) + jnp.where(span == rank + kvec, b, 0.0)
        red1[i, 0] = jnp.sum(both, axis=0, keepdims=True)
        pair_copy(i).start()

    def red_mid(i):
        pair_copy(i).wait_recv()
        red2[i, lax.div(me, 2)] = red1[i, 0] + red1[i, 1]

        for j in range(1, others):
            chip_copy(i, j).start()

    def red_end(i):
        got = red2.at[i, pl.ds(0, others - 1)]
        pltpu.make_async_copy(got, got, r2r.at[i]).wait()
        pltpu.make_async_copy(got, got, r2s.at[i]).wait()
        pair_copy(i).wait_send()
        line = jnp.broadcast_to(jnp.sum(red2[i], axis=0), (kvec, 128))
        top = jnp.sum(jnp.where(span == rank, line, 0.0), axis=1, keepdims=True)
        bottom = jnp.sum(jnp.where(span == rank + kvec, line, 0.0), axis=1, keepdims=True)
        return top, bottom

    class Exchange:
        def __init__(self, src, near, far, out, sems):
            self.src, self.near, self.far, self.out, self.sems = src, near, far, out, sems

        def near_copy(self, j):
            to = lax.rem(low + j, LOW)
            return rcopy(self.src.at[to], self.near.at[low], self.sems[0].at[j], self.sems[1].at[low], high * LOW + to)

        def near_in(self, j):
            frm = lax.rem(low + j, LOW)
            return rcopy(self.src.at[frm], self.near.at[frm], self.sems[0].at[j], self.sems[1].at[frm], left)

        def far_copy(self, j):
            to = lax.rem(high + j, n_high) * LOW + low
            return rcopy(self.far.at[high], self.far.at[high], self.sems[2].at[j], self.sems[3].at[high], to)

        def far_in(self, j):
            frm = lax.rem(high + j, n_high)
            return rcopy(self.far.at[frm], self.far.at[frm], self.sems[2].at[j], self.sems[3].at[frm], left)

        def back_copy(self, j):
            to = high * LOW + lax.rem(low + j, LOW)
            return rcopy(self.out.at[low], self.out.at[low], self.sems[4].at[j], self.sems[5].at[low], to)

        def back_in(self, j):
            frm = lax.rem(low + j, LOW)
            return rcopy(self.out.at[frm], self.out.at[frm], self.sems[4].at[j], self.sems[5].at[frm], left)

        def start(self):
            for j in range(1, LOW):
                self.near_copy(j).start()
            self.near[low] = self.src[low]

        def middle(self):
            for j in range(1, LOW):
                self.near_in(j).wait_recv()
            tile = self.near[0]
            for l in range(1, LOW):
                tile = tile + self.near[l]
            self.far[high] = tile
            for j in range(1, n_high):
                self.far_copy(j).start()

        def back(self):
            for j in range(1, n_high):
                self.far_in(j).wait_recv()
            tile = self.far[0]
            for l in range(1, n_high):
                tile = tile + self.far[l]
            self.out[low] = tile
            for j in range(1, LOW):
                self.back_copy(j).start()

        def end(self):
            for j in range(1, LOW):
                self.back_in(j).wait_recv()

        def drain(self):
            for j in range(1, LOW):
                self.near_copy(j).wait_send()
                self.back_copy(j).wait_send()
            for j in range(1, n_high):
                self.far_copy(j).wait_send()

    soon = Exchange(early, early1, early2, early3, (e1s, e1r, e2s, e2r, e3s, e3r))
    later = Exchange(parts, big1, big2, fin, (b1s, b1r, b2s, b2r, b3s, b3r))

    class Apply:
        def __init__(self, kv, parts_ref, acc_ref):
            self.kv, self.zs, self.acc = kv, parts_ref, acc_ref

        def put(self, b, z):
            zh, zl = split(z)
            self.zs[b, 0:self.kv, :] = zh
            self.zs[b, self.kv:2 * self.kv, :] = zl

        def diag(self, b, z):
            self.acc[b] = onsite[b] * z

        def clear_tail(self):
            for t in range(HB):
                self.acc[rows + t] = jnp.zeros((self.kv, bs), F32)

        def product(self, z, hi, lo):
            part = mm(z, hi)
            return part[0:self.kv] + part[self.kv:] + mm(z[0:self.kv], lo)

        def onto(self, b):
            zb = self.zs[b]
            moved = [self.product(zb, bh[b * SLOTS + s], bl[b * SLOTS + s]) for s in range(SLOTS)]
            for o in range(HB + 1):
                total_o = self.acc[b + o]
                for s in range(SLOTS):
                    total_o = total_o + jnp.where(offs[b * SLOTS + s] == o, 1.0, 0.0) * moved[s]
                self.acc[b + o] = total_o

        def across(self, b):
            out = None
            for s in range(SLOTS):
                term = self.product(self.zs[b + offs[b * SLOTS + s]], th[b * SLOTS + s], tl[b * SLOTS + s])
                out = term if out is None else out + term
            self.acc[b] = self.acc[b] + out

        def halo_in(self, n):
            z_copy(n).wait_recv()
            for t in range(HB):
                self.put(rows + t, zhalo0[t] if n == 0 else zhalo[n - 1, t])

        def send_spill(self, n):
            for t in range(HB):
                if n == 0:
                    spill0[t] = self.acc[rows + t]
                else:
                    spill[n - 1, t] = self.acc[rows + t]
            spill_copy(n).start()

        def take_in(self, n):
            spill_copy(n).wait_recv()
            for t in range(HB):
                self.acc[t] = self.acc[t] + (inc0[t] if n == 0 else inc[n - 1, t])

    wide = Apply(2 * kvec, zsw, accw)
    thin = Apply(kvec, zs, acc)

    def precondition(x, b):
        dh, dl = split(x)
        part = mm(jnp.concatenate([dh, dl], axis=0), ph[b])
        return part[0:kvec] + part[kvec:] + mm(dh, plo[b])

    pltpu.make_async_copy(fw.at[:, pl.ds(0, kvec)], fw.at[:, pl.ds(0, kvec)], load_sem.at[0]).wait()
    for copy in smalls:
        copy.wait()
    for j in range(rows // SLOTS):
        precond_copy(j).wait()
        for t in range(SLOTS):
            b = j * SLOTS + t
            xh, xl = split(stage[j, t])
            ph[b] = xh.T
            plo[b] = xl.T
        block_copy(edge + j, j).start()
        for t in range(SLOTS):
            b = j * SLOTS + t
            v = fw[b, 0:kvec]
            fw[b, kvec:2 * kvec] = precondition(v, b)
            x = fw[b]
            wide.put(b, x)
            wide.diag(b, x)
    lax.fori_loop(0, rows, start_more, 0)
    wide.clear_tail()

    def take_row(b, slot):
        block_copy(b, slot).wait()
        for s in range(SLOTS):
            off = cols[s, b] - first - b
            off = jnp.where(off < 0, off + total, off)
            offs[b * SLOTS + s] = jnp.minimum(off, HB)
            alive = jnp.where(s < live[b], 1.0, 0.0)
            xh, xl = split(stage[slot, s] * alive)
            bh[b * SLOTS + s] = xh
            bl[b * SLOTS + s] = xl
            th[b * SLOTS + s] = bh[b * SLOTS + s].T
            tl[b * SLOTS + s] = bl[b * SLOTS + s].T

    def tail_row(i, c):
        take_row(edge + i, i)
        block_copy(i, i).start()
        wide.onto(edge + i)
        return c

    lax.fori_loop(0, HB, tail_row, 0)
    pl.semaphore_wait(barrier, n_greet)
    z_copy(0).start()
    wide.send_spill(0)

    def head_row(b, c):
        slot = lax.rem(b, STAGES)
        take_row(b, slot)

        @pl.when(b + STAGES < edge)
        def _():
            block_copy(b + STAGES, slot).start()

        wide.onto(b)
        wide.across(b)
        return c

    lax.fori_loop(0, edge, head_row, 0)
    wide.halo_in(0)
    for b in range(edge, rows):
        wide.across(b)
    wide.take_in(0)

    zero = jnp.zeros((kvec, bs), F32)

    def first_sums(b, c):
        x = fw[b, 0:kvec]
        im = accw[b, 0:kvec]
        fim[b] = im
        fhw[b] = accw[b, kvec:2 * kvec]
        return c[0] + x * im, c[1] + x * x

    num, den = lax.fori_loop(0, rows, first_sums, (zero, zero))
    total_of = lambda x: jnp.sum(x, axis=1, keepdims=True)
    red_start(0, total_of(num), total_of(den))

    pltpu.make_async_copy(fpv, fpv, load_sem.at[1]).wait()
    pltpu.make_async_copy(fpi, fpi, load_sem.at[2]).wait()

    def old_products(b, c):
        xh, xl = split(jnp.concatenate([fw[b, 0:kvec], fpv[b], fim[b], fpi[b]], axis=0))
        m = 2 * kvec
        part = mmt(jnp.concatenate([xh[0:m], xl[0:m]], axis=0), xh)
        return c + (part[0:m] + part[m:] + mmt(xh[0:m], xl))

    old = lax.fori_loop(0, rows, old_products, jnp.zeros((2 * kvec, 128), F32))
    for p in range(8):
        early[p] = old[8 * p:8 * p + 8]
    soon.start()

    for k in range(ITERS):
        n = k + 1
        field = fim if k == 0 else fa

        def prepare(b, field=field):
            z = precondition(field[b], b)
            fz[b] = z
            thin.put(b, z)
            thin.diag(b, z)

        for b in range(HB):
            prepare(b)
        z_copy(n).start()
        thin.clear_tail()
        for b in range(edge, rows):
            prepare(b)
        red_mid(k)
        for b in range(edge, rows):
            thin.onto(b)
        thin.send_spill(n)

        def interior(g, c, prepare=prepare):
            for t in range(4):
                prepare(4 + 4 * g + t)
            return c

        for g in range((edge - HB) // 4):
            interior(g, 0)

        def body(g, c):
            for t in range(4):
                thin.onto(4 * g + t)
            for t in range(4):
                thin.across(4 * g + t)
            return c

        for g in range(edge // 4):
            body(g, 0)
        thin.halo_in(n)
        for b in range(edge, rows):
            thin.across(b)
        thin.take_in(n)
        z_copy(n).wait_send()
        (soon.middle, soon.back, soon.end)[k]()
        top, bottom = red_end(k)
        if k == 0:
            qb[...] = jnp.broadcast_to(top / bottom, (kvec, bs))
        else:
            sb[...] = jnp.broadcast_to(top / (bottom + 1.0), (kvec, bs))

        def update(b, c, k=k):
            z, hz = fz[b], acc[b]
            q = qb[...]
            if k == 0:
                u = q * fw[b, kvec:2 * kvec] - z
                hu = q * fhw[b] - hz
                r = q * fw[b, 0:kvec] - fim[b]
                a = hu - q * u
                fu[b] = u
                fhu[b] = hu
                fr[b] = r
            else:
                m = hz - q * z
                s = sb[...]
                u, hu, a = fu[b], fhu[b], fa[b]
                r = fr[b] - s * a
                fr[b] = r
                if k == 1:
                    fc[b] = s * u
                    fh[b] = s * hu
                else:
                    fc[b] = fc[b] + s * u
                    fh[b] = fh[b] + s * hu
                a = a - s * m
                fu[b] = u - s * z
                fhu[b] = hu - s * hz
            fa[b] = a
            return c[0] + a * r, c[1] + a * a

        cross, own = lax.fori_loop(0, rows, update, (zero, zero))
        if k + 1 < ITERS:
            red_start(k + 1, total_of(cross), total_of(own))

    def put_out(b, c):
        at = pl.ds(pl.multiple_of(b * bs, bs), bs)
        pltpu.make_async_copy(fc.at[b], c_out.at[:, at], out_sem.at[0]).start()
        pltpu.make_async_copy(fu.at[b], u_out.at[:, at], out_sem.at[1]).start()
        return c

    red_start(ITERS, total_of(cross), total_of(own))
    lax.fori_loop(0, rows, put_out, 0)

    def product_of(b):
        xh, xl = split(jnp.concatenate([fw[b, 0:kvec], fpv[b], fc[b], fu[b]], axis=0))
        yh, yl = split(jnp.concatenate([fim[b], fpi[b], fh[b], fhu[b]], axis=0))
        m = 2 * kvec
        n = 2 * m
        left_side = jnp.concatenate([xh[m:], yh[m:], xl[m:], yl[m:]], axis=0)
        part = mmt(left_side, jnp.concatenate([xh, yh], axis=0))
        return part[0:n], part[n:], mmt(left_side[0:n], jnp.concatenate([xl, yl], axis=0))

    gram[...] = jnp.zeros_like(gram)

    def products(g, c):
        one, two = product_of(2 * g), product_of(2 * g + 1)
        gram[...] = gram[...] + ((one[0] + two[0]) + (one[1] + two[1]) + (one[2] + two[2]))
        return c

    lax.fori_loop(0, rows // 2, products, 0)
    hp = pltpu.roll(gram[2 * kvec:3 * kvec, 0:128], 64, 1)
    hup = pltpu.roll(gram[3 * kvec:4 * kvec, 0:128], 64, 1)
    last = span >= 3 * kvec
    quarters = (
        jnp.where(last, hp, gram[0:kvec, 0:128]),
        gram[kvec:2 * kvec, 0:128],
        jnp.where(last, hup, gram[0:kvec, 128:256]),
        gram[kvec:2 * kvec, 128:256],
    )
    for p in range(4):
        parts[2 * p] = quarters[p][0:kvec // 2]
        parts[2 * p + 1] = quarters[p][kvec // 2:]
    later.start()
    red_mid(ITERS)
    later.middle()
    top, bottom = red_end(ITERS)
    sums_out[...] = jnp.broadcast_to(top / (bottom + 1.0), (kvec, 128))
    later.back()
    for p in range(8):
        early_out[p] = early3[p]
    later.end()
    for p in range(8):
        late_out[p] = fin[p]
    pltpu.make_async_copy(fc, fc, out_sem.at[0]).wait()
    pltpu.make_async_copy(fu, fu, out_sem.at[1]).wait()

    soon.drain()
    later.drain()
    z_copy(0).wait_send()
    for n in range(ITERS + 1):
        spill_copy(n).wait_send()


def finish(kvec, c_in, u_in, early, late, step_in, corr, reduced, cbuf, ubuf, aug, sem):
    first = pltpu.make_async_copy(c_in, cbuf, sem.at[0])
    second = pltpu.make_async_copy(u_in, ubuf, sem.at[1])
    third = pltpu.make_async_copy(cbuf, corr, sem.at[2])
    first.start()
    second.start()
    step = step_in[:, 0:1]

    def add_last():
        wide = jnp.broadcast_to(step, (kvec, 512))
        first.wait()
        second.wait()

        def add(g, c):
            at = pl.ds(pl.multiple_of(g * 512, 512), 512)
            cbuf[:, at] = cbuf[:, at] + wide * ubuf[:, at]
            return c

        lax.fori_loop(0, cbuf.shape[1] // 512, add, 0)
        third.start()

    quarter = lambda p: jnp.concatenate([late[2 * p], late[2 * p + 1]], axis=0)
    half = lambda g: jnp.concatenate([early[4 * g + p] for p in range(4)], axis=0)
    full = reduce_basis([half(0), half(1)], [quarter(p) for p in range(4)], step, aug, kvec, add_last)
    reduced[...] = full[:, 0:3 * kvec]
    third.wait()


def local(n_dev, blocks, block_cols, live_counts, onsite_energy, precond, vectors, prev_vectors, prev_image):
    rows, slots, bs = blocks.shape[0], blocks.shape[1], blocks.shape[2]
    kvec = vectors.shape[0]
    n_high = n_dev // LOW
    field = pltpu.VMEM((rows, kvec, bs), F32)
    tiles = pltpu.VMEM((rows * slots, bs, bs), BF16)
    dma = pltpu.SemaphoreType.DMA
    hbm = pl.BlockSpec(memory_space=pl.ANY)
    vmem = pl.BlockSpec(memory_space=pltpu.VMEM)

    def run(*args):
        return kernel(n_dev, rows, kvec, bs, *args)

    outs = pl.pallas_call(
        run,
        out_shape=(
            jax.ShapeDtypeStruct(vectors.shape, F32),
            jax.ShapeDtypeStruct(vectors.shape, F32),
            jax.ShapeDtypeStruct((8, 8, 128), F32),
            jax.ShapeDtypeStruct((8, kvec // 2, 128), F32),
            jax.ShapeDtypeStruct((kvec, 128), F32),
        ),
        in_specs=[hbm] * 8,
        out_specs=(hbm, hbm, vmem, vmem, vmem),
        scratch_shapes=[
            pltpu.SMEM((slots, rows), jnp.int32),
            pltpu.SMEM((rows,), jnp.int32),
            pltpu.VMEM((rows, 1, bs), F32),
            pltpu.VMEM((STAGES, slots, bs, bs), F32),
            tiles, tiles, tiles, tiles,
            pltpu.VMEM((rows, bs, bs), BF16),
            pltpu.VMEM((rows, bs, bs), BF16),
            pltpu.SMEM((rows * slots,), jnp.int32),
            pltpu.VMEM((rows, 2 * kvec, bs), F32),
            field, field, field, field, field, field, field, field, field, field, field,
            pltpu.VMEM((rows + HB, 4 * kvec, bs), BF16),
            pltpu.VMEM((rows + HB, 2 * kvec, bs), F32),
            pltpu.VMEM((rows + HB, 2 * kvec, bs), BF16),
            pltpu.VMEM((rows + HB, kvec, bs), F32),
            pltpu.VMEM((kvec, bs), F32),
            pltpu.VMEM((kvec, bs), F32),
            pltpu.VMEM((ITERS, HB, kvec, bs), F32),
            pltpu.VMEM((ITERS, HB, kvec, bs), F32),
            pltpu.VMEM((ITERS, HB, kvec, bs), F32),
            pltpu.VMEM((HB, 2 * kvec, bs), F32),
            pltpu.VMEM((HB, 2 * kvec, bs), F32),
            pltpu.VMEM((HB, 2 * kvec, bs), F32),
            pltpu.VMEM((ITERS + 1, 2, 1, 128), F32),
            pltpu.VMEM((ITERS + 1, n_dev // 2, 1, 128), F32),
            pltpu.VMEM((4 * kvec, 256), F32),
            pltpu.VMEM((LOW, 8, 128), F32),
            pltpu.VMEM((LOW, 8, 128), F32),
            pltpu.VMEM((n_high, 8, 128), F32),
            pltpu.VMEM((LOW, 8, 128), F32),
            pltpu.VMEM((LOW, kvec // 2, 128), F32),
            pltpu.VMEM((LOW, kvec // 2, 128), F32),
            pltpu.VMEM((n_high, kvec // 2, 128), F32),
            pltpu.VMEM((LOW, kvec // 2, 128), F32),
            dma((STAGES,)), dma((6,)), dma((2,)),
            dma((ITERS + 1,)), dma((ITERS + 1,)), dma((ITERS + 1,)), dma((ITERS + 1,)),
            dma((ITERS + 1,)), dma((ITERS + 1,)), dma((ITERS + 1,)), dma((ITERS + 1,)),
            dma((LOW,)), dma((LOW,)), dma((n_high,)), dma((n_high,)), dma((LOW,)), dma((LOW,)),
            dma((LOW,)), dma((LOW,)), dma((n_high,)), dma((n_high,)), dma((LOW,)), dma((LOW,)),
        ],
        compiler_params=pltpu.CompilerParams(
            collective_id=0, has_side_effects=True, vmem_limit_bytes=63 * 1024 * 1024
        ),
    )(block_cols.T, live_counts, blocks, onsite_energy.reshape(rows, 1, bs), precond, vectors, prev_vectors, prev_image)

    def run_last(*args):
        return finish(kvec, *args)

    return pl.pallas_call(
        run_last,
        out_shape=(
            jax.ShapeDtypeStruct(vectors.shape, F32),
            jax.ShapeDtypeStruct((3 * kvec, 3 * kvec), F32),
        ),
        in_specs=[hbm, hbm, vmem, vmem, vmem],
        out_specs=(hbm, vmem),
        scratch_shapes=[
            pltpu.VMEM(vectors.shape, F32),
            pltpu.VMEM(vectors.shape, F32),
            pltpu.VMEM((3 * kvec, 256), F32),
            dma((3,)),
        ],
    )(*outs)


def solution(mesh):
    n_dev = mesh.shape["rows"]

    def step(*args):
        return local(n_dev, *args)

    return jax.shard_map(
        step,
        mesh=mesh,
        in_specs=(
            P("rows", None, None, None), P("rows", None), P("rows"), P("rows"),
            P("rows", None, None), P(None, "rows"), P(None, "rows"), P(None, "rows"),
        ),
        out_specs=(P(None, "rows"), P()),
        check_vma=False,
    )
```
